32 devices in a mesh: expert: 8 (over z, y), dp: 4 (over x, core).
Axes of the slice: x: 2, y: 2, z: 4, core: 2. Of those that a mesh axis runs over, the one named last changes fastest.
Arguments:
- tokens: bfloat16 [2048, 2880], P(('expert', 'dp')), may hold values from -6 to 6
- expert_ids: int32 [2048, 4], P(('expert', 'dp')), may hold values from 0 to 7, all different within a row; in each aligned block of 64 rows (0 to 63, 64 to 127, ...) at most 48 rows name the same one
- gate_logits: float32 [2048, 4], P(('expert', 'dp')), may hold values from -3 to 3
- w_gate: bfloat16 [8, 2880, 1536], P('expert', None, 'dp'), may hold values from -0.109375 to 0.109375
- w_up: bfloat16 [8, 2880, 1536], P('expert', None, 'dp'), may hold values from -0.109375 to 0.109375
- w_down: bfloat16 [8, 1536, 2880], P('expert', 'dp'), may hold values from -0.15625 to 0.15625
Outputs:
- mixed: bfloat16 [2048, 2880], P(('expert', 'dp'))
The draws below stay inside these ranges and needn't reach their ends.
Inputs may be any that keep to these rules, and one draw needn't show every extreme that they name: `expert_ids`: each row names 4 different experts. Among the 64 rows of one device no expert is named more than 48 times, and every expert is named somewhere.
All inputs are finite; a program needn't handle non-finite values.
Results may differ from the reference program's by a relative error of at most 0.012.
Values may be sent and summed in bfloat16 or wider, within the bound.
A program may use at most 128 MiB of HBM per device.

```python
import math
import jax
import jax.numpy as jnp
import numpy as np
from jax import lax

D = 2880
FF = 1536
TOP = 4
TOK_DEV = 64
EXPERTS = 8
CAP = 48
TOKENS = 2048
N_EXPERT = 8
N_DP = 4


def levels(rng, dims, split, smallest, largest):
    loudness, own = 1.0, jax.random.fold_in(rng, 6)
    for dim, shards_of in split:
        steps = jnp.exp(jax.random.uniform(jax.random.fold_in(own, dim), (shards_of,), jnp.float32, smallest / len(split), largest / len(split)))
        loudness = loudness * jnp.repeat(steps, dims[dim] // shards_of).reshape([-1 if axis == dim else 1 for axis in range(len(dims))])
    return loudness


def shared_out(key, own, number, rows, count, top, most, lean):
    order = jax.random.permutation(key, count)
    crowded, common = shares(count, rows * top, most, lean, True), shares(count, rows * top, most, lean, False)
    places = jnp.arange(count)

    def named(tallies, rotation):
        used = int((tallies > 0).sum())
        fixed = max(1, used // 4)
        moved = fixed + (places - fixed + rotation * (used - fixed)) % max(1, count - fixed)
        return jnp.zeros((count,), jnp.int32).at[order[jnp.where(places < fixed, places, moved)]].set(jnp.asarray(tallies, jnp.int32))

    tallies = jnp.where(number % 4 == 0, named(crowded, number // 4), named(common, number - number // 4 - 1))
    mixed = jax.random.permutation(jax.random.fold_in(own, 3), count)
    source_of, taker = mixed[0:count // 2 * 2:2], mixed[1:count // 2 * 2:2]
    room = jnp.minimum(tallies[source_of] - 1, most - tallies[taker]) // 2
    room = jnp.where((source_of == order[0]) | (taker == order[0]) | (tallies[taker] == 0), 0, jnp.maximum(room, 0))
    moved = jax.random.randint(jax.random.fold_in(own, 4), (count // 2,), 0, 1 << 20) % (room + 1)
    tallies = tallies.at[source_of].add(-moved).at[taker].add(moved)
    labels = jnp.searchsorted(jnp.cumsum(tallies), jnp.arange(rows * top), side="right").astype(jnp.int32)
    table = labels.reshape(top, rows).T
    table = table[jax.random.permutation(jax.random.fold_in(own, 1), rows)]
    rotation = jax.random.randint(jax.random.fold_in(own, 2), (rows, 1), 0, top)
    return jnp.take_along_axis(table, (jnp.arange(top)[None, :] + rotation) % top, axis=1)


def shares(amount, total, limit, skew, full):
    weights = [(1 << 20) // math.isqrt(standing ** skew) + 1 for standing in range(1, amount + 1)]
    largest = limit if full else min(limit, max(-(-total // amount), total * weights[0] // sum(weights)))
    least = 1 if total - largest >= amount - 1 else 0
    given, spare = [largest] + [least] * (amount - 1), total - largest - least * (amount - 1)
    while spare > 0:
        movable = [i for i in range(1, amount) if given[i] < largest] or [i for i in range(1, amount) if given[i] < limit]
        mass, left = sum([weights[i] for i in movable]), spare
        for i in movable:
            addition = min(limit - given[i], max(1, left * weights[i] // mass), spare)
            given[i] = given[i] + addition
            spare = spare - addition
    return np.array(given)


def normal_values(key, extent, scale, most, split=(), kind=jnp.bfloat16):
    result = jax.random.normal(key, extent, jnp.float32) * scale
    if len(split) > 0:
        result = levels(key, extent, split, -0.22, 0.18) * result
    return jnp.clip(result, min=-most, max=most).astype(kind)


def setup_inputs(seed: int = 0) -> dict:
    key_list = jax.random.split(jax.random.key(seed), 7)
    tokens = normal_values(key_list[0], (TOKENS, D), 1.0, 6.0, ((0, 32),))
    expert_ids_keys = jax.random.split(jax.random.fold_in(key_list[1], 1), TOKENS // TOK_DEV)
    expert_ids_turns = jax.random.permutation(jax.random.fold_in(key_list[1], 3), TOKENS // TOK_DEV)
    expert_ids = jax.vmap(lambda own, number: shared_out(jax.random.fold_in(key_list[1], 2), own, number, TOK_DEV, EXPERTS, TOP, CAP, 2))(expert_ids_keys, expert_ids_turns).reshape((TOKENS, TOP))
    gate_logits = jnp.clip(jax.random.uniform(key_list[2], (TOKENS, TOP), jnp.float32, -3.0, 3.0) * levels(key_list[2], (TOKENS, TOP), ((0, 32),), -0.4, 0.0), -3.0, 3.0)
    w_gate = normal_values(key_list[3], (EXPERTS, D, FF), D ** -0.5, 0.109375, ((0, 8), (2, 4)))
    w_up = normal_values(key_list[4], (EXPERTS, D, FF), D ** -0.5, 0.109375, ((0, 8), (2, 4)))
    w_down = normal_values(key_list[5], (EXPERTS, FF, D), FF ** -0.5, 0.15625, ((0, 8), (1, 4)))
    return dict(tokens=tokens, expert_ids=expert_ids, gate_logits=gate_logits, w_gate=w_gate, w_up=w_up, w_down=w_down)


def expert_rows(rows_in, gate_w, up_w, down_w):
    quarter = gate_w.shape[1] // N_DP
    summed = jnp.zeros((rows_in.shape[0], down_w.shape[1]), jnp.float32)
    for index_q in range(N_DP):
        low_col = index_q * quarter
        high_col = low_col + quarter
        gate_val = jnp.dot(rows_in, gate_w[:, low_col:high_col], preferred_element_type=jnp.float32)
        up_val = jnp.dot(rows_in, up_w[:, low_col:high_col], preferred_element_type=jnp.float32)
        hidden = ((up_val + 1.0) * gate_val * jax.nn.sigmoid(1.702 * gate_val)).astype(jnp.bfloat16)
        partial_value = jnp.dot(hidden, down_w[low_col:high_col], preferred_element_type=jnp.float32).astype(jnp.bfloat16)
        summed = summed + lax.optimization_barrier(partial_value).astype(jnp.float32)
    return summed.astype(jnp.bfloat16)


def reference(tokens, expert_ids, gate_logits, w_gate, w_up, w_down):
    n_assign = TOKENS * TOP
    flat_ids = expert_ids.reshape(-1).astype(jnp.int32)
    sorter = jnp.argsort(flat_ids, stable=True).astype(jnp.int32)
    counts = jnp.sum((flat_ids[:, None] == jnp.arange(EXPERTS, dtype=jnp.int32)[None, :]).astype(jnp.int32), axis=0)
    starts = (jnp.cumsum(counts) - counts).astype(jnp.int32)
    longest = N_EXPERT * N_DP * CAP
    padded_order = jnp.concatenate([sorter, jnp.zeros((longest,), jnp.int32)])

    def per_expert(expert):
        chosen = lax.dynamic_slice_in_dim(padded_order, starts[expert], longest)
        rows_in = tokens[chosen // TOP]
        return expert_rows(rows_in, w_gate[expert], w_up[expert], w_down[expert])

    outputs_all = lax.map(per_expert, jnp.arange(EXPERTS, dtype=jnp.int32))
    inverse = jnp.zeros((n_assign,), jnp.int32).at[sorter].set(jnp.arange(n_assign, dtype=jnp.int32))
    rank_in = (inverse - starts[flat_ids]).astype(jnp.int32)
    picked = outputs_all.reshape(-1, D)[flat_ids * longest + rank_in]
    gate_wts = jnp.exp(gate_logits.astype(jnp.float32))
    gate_wts = gate_wts / jnp.sum(gate_wts, axis=1, keepdims=True)
    mixed = jnp.sum(picked.reshape(TOKENS, TOP, D).astype(jnp.float32) * gate_wts[:, :, None], axis=1)
    return mixed.astype(jnp.bfloat16)
```

```python
import functools

import jax
import jax.numpy as jnp
from jax import lax
from jax.experimental import pallas as pl
from jax.experimental.pallas import tpu as pltpu
from jax.sharding import PartitionSpec as P


def expert_rows(tile_in, gate_w, up_w, down_w):
    gate_val = jnp.dot(tile_in, gate_w, preferred_element_type=jnp.float32)
    up_val = jnp.dot(tile_in, up_w, preferred_element_type=jnp.float32)
    hidden = ((up_val + 1.0) * gate_val * jax.nn.sigmoid(1.702 * gate_val)).astype(jnp.bfloat16)
    return jnp.dot(hidden, down_w, preferred_element_type=jnp.float32).astype(jnp.bfloat16)


def run_tiles(packed, first_row, last_row, gate_w, up_w, down_w):
    tile_rows = 128
    n_tiles = jnp.maximum(last_row - first_row + tile_rows - 1, 0) // tile_rows
    result_buf = jnp.zeros((packed.shape[0], down_w.shape[1]), jnp.bfloat16)

    def advance(index_t, buffer):
        at_row = first_row + index_t * tile_rows
        tile_in = lax.dynamic_slice_in_dim(packed, at_row, tile_rows, 0)
        return lax.dynamic_update_slice_in_dim(
            buffer, expert_rows(tile_in, gate_w, up_w, down_w), at_row, 0
        )

    return lax.fori_loop(0, n_tiles, advance, result_buf)


def sparse_device(tokens, expert_ids, gate_logits, w_gate, w_up, w_down):
    n_rows, width = tokens.shape
    n_tops = expert_ids.shape[1]
    n_exp = lax.axis_size("expert")
    n_dp = lax.axis_size("dp")
    slot_cap = max(2, 3 * n_rows * n_tops // (2 * n_exp))
    tile_rows = 128
    flat_ids = expert_ids.reshape(-1)
    onehot = (flat_ids[:, None] == jnp.arange(n_exp, dtype=jnp.int32)[None, :]).astype(jnp.int32)
    rank_in = jnp.sum((jnp.cumsum(onehot, axis=0) - onehot) * onehot, axis=1)
    counts = jnp.sum(onehot, axis=0)
    slot_idx = flat_ids * slot_cap + rank_in
    source = (
        jnp.zeros((n_exp * slot_cap,), jnp.int32)
        .at[slot_idx]
        .set(jnp.arange(n_rows * n_tops, dtype=jnp.int32) // n_tops)
    )
    filled = (jnp.arange(slot_cap)[None, :] < counts[:, None]).reshape(-1)
    outgoing = jnp.where(filled[:, None], tokens[source], jnp.zeros_like(tokens[source])).reshape(
        n_exp, slot_cap, width
    )
    rows_mid, counts_mid = (
        lax.all_to_all(outgoing, "expert", split_axis=0, concat_axis=0, tiled=True),
        lax.all_to_all(counts[:, None], "expert", split_axis=0, concat_axis=0, tiled=True),
    )
    rows_in, counts_in = (
        lax.all_gather(rows_mid, "dp", axis=0, tiled=True),
        lax.all_gather(counts_mid, "dp", axis=0, tiled=True),
    )
    rows_flat = rows_in.reshape(-1, width)
    total_rows = rows_flat.shape[0]
    live_row = (jnp.arange(slot_cap)[None, :] < counts_in.reshape(-1)[:, None]).reshape(-1)
    position = jnp.cumsum(live_row.astype(jnp.int32)) - 1
    live_total = jnp.sum(live_row.astype(jnp.int32))
    padded = (total_rows + tile_rows - 1) // tile_rows * tile_rows + tile_rows
    gather_idx = (
        jnp.zeros((padded,), jnp.int32)
        .at[jnp.where(live_row, position, padded)]
        .set(jnp.arange(total_rows, dtype=jnp.int32), mode="drop")
    )
    packed = rows_flat[gather_idx]
    gate_w = w_gate[0]
    up_w = w_up[0]
    down_w = w_down[0]
    merged = run_tiles(packed, 0, live_total, gate_w, up_w, down_w)
    slot_out = jnp.where(
        live_row[:, None],
        merged[jnp.where(live_row, position, 0)],
        jnp.zeros((total_rows, width), jnp.bfloat16),
    )
    summed = lax.psum_scatter(
        slot_out.reshape(n_dp * n_exp, slot_cap, width), "dp", scatter_dimension=0, tiled=True
    ).astype(jnp.float32)
    expert_out = lax.all_to_all(
        summed.astype(jnp.bfloat16), "expert", split_axis=0, concat_axis=0, tiled=True
    )
    picked = expert_out.reshape(n_exp * slot_cap, width)[slot_idx]
    gate_wts = jnp.exp(gate_logits)
    gate_wts = gate_wts / jnp.sum(gate_wts, axis=1, keepdims=True)
    mixed = jnp.sum(
        picked.reshape(n_rows, n_tops, width).astype(jnp.float32) * gate_wts[:, :, None], axis=1
    )
    return mixed.astype(jnp.bfloat16)


LANES = 128
CHUNKS = 1


def round_up(value, step):
    return (value + step - 1) // step * step


def routing_columns(expert_ids, gate_logits, n_exp, lanes):
    gate_wts = jnp.exp(gate_logits)
    gate_wts = gate_wts / jnp.sum(gate_wts, axis=1, keepdims=True)
    chosen = expert_ids[:, :, None] == jnp.arange(n_exp, dtype=jnp.int32)[None, None, :]
    by_expert = jnp.sum(jnp.where(chosen, gate_wts[:, :, None], 0.0), axis=1)
    high = by_expert.astype(jnp.bfloat16)
    low = (by_expert - high.astype(jnp.float32)).astype(jnp.bfloat16)
    columns = jnp.concatenate([high, low], axis=1)
    return jnp.pad(columns, ((0, 0), (0, lanes - columns.shape[1])))


def dense_kernel(n_exp, rows_ref, gate_ref, up_ref, down_ref, out_ref):
    width, hidden_width = gate_ref.shape
    lanes = rows_ref.shape[1]
    mine = lax.axis_index("expert")
    rows_in = rows_ref[:, :width]
    gate_val = jnp.dot(rows_in, gate_ref[...], preferred_element_type=jnp.float32)
    up_val = jnp.dot(rows_in, up_ref[...], preferred_element_type=jnp.float32)
    first = width // LANES * LANES
    extra = rows_ref[:, first:lanes].astype(jnp.float32)
    lane = lax.broadcasted_iota(jnp.int32, extra.shape, 1) + first - width
    weight = jnp.sum(jnp.where((lane == mine) | (lane == mine + n_exp), extra, 0.0), axis=1, keepdims=True)
    hidden = (up_val + 1.0) * gate_val * (weight / (1.0 + jnp.exp(-1.702 * gate_val)))
    out_ref[...] = jnp.dot(
        hidden.astype(jnp.bfloat16), down_ref[...], preferred_element_type=jnp.float32
    ).astype(out_ref.dtype)


def dense_rows(rows, gate_w, up_w, down_w, n_exp):
    n_rows, lanes = rows.shape
    width, hidden_width = gate_w.shape
    tile_rows = 256
    while n_rows % tile_rows:
        tile_rows //= 2
    whole = pl.BlockSpec(memory_space=pltpu.VMEM)
    return pl.pallas_call(
        functools.partial(dense_kernel, n_exp),
        grid=(n_rows // tile_rows,),
        in_specs=[pl.BlockSpec((tile_rows, lanes), lambda i: (i, 0)), whole, whole, whole],
        out_specs=pl.BlockSpec((tile_rows, width), lambda i: (i, 0)),
        out_shape=jax.ShapeDtypeStruct((n_rows, width), jnp.bfloat16),
        cost_estimate=pl.CostEstimate(
            flops=6 * n_rows * width * hidden_width,
            bytes_accessed=2 * n_rows * (lanes + width) + 6 * width * hidden_width,
            transcendentals=n_rows * hidden_width,
        ),
    )(rows, gate_w, up_w, down_w)


def dense_device(tokens, expert_ids, gate_logits, w_gate, w_up, w_down):
    n_rows, width = tokens.shape
    n_exp = lax.axis_size("expert")
    both = ("expert", "dp")
    lanes = round_up(width + 2 * n_exp, LANES)
    extra = routing_columns(expert_ids, gate_logits, n_exp, lanes - width)
    wide = jnp.concatenate([tokens, extra], axis=1)
    step = n_rows // CHUNKS
    done = []
    for chunk in range(CHUNKS):
        rows = lax.all_gather(wide[chunk * step : (chunk + 1) * step], both, axis=0, tiled=True)
        partial = dense_rows(rows, w_gate[0], w_up[0], w_down[0], n_exp)
        done.append(lax.psum_scatter(partial, both, scatter_dimension=0, tiled=True))
    return done[0] if CHUNKS == 1 else jnp.concatenate(done, axis=0)


def tile_product(n_exp, rows_in, extra, gate_ref, up_ref, down_ref):
    width = gate_ref.shape[0]
    mine = lax.axis_index("expert")
    gate_val = jnp.dot(rows_in, gate_ref[...], preferred_element_type=jnp.float32)
    up_val = jnp.dot(rows_in, up_ref[...], preferred_element_type=jnp.float32)
    extra = extra.astype(jnp.float32)
    lane = lax.broadcasted_iota(jnp.int32, extra.shape, 1) - width % LANES
    weight = jnp.sum(jnp.where((lane == mine) | (lane == mine + n_exp), extra, 0.0), axis=1, keepdims=True)
    hidden = (up_val + 1.0) * gate_val * (weight / (1.0 + jnp.exp(-1.702 * gate_val)))
    return lax.dot_general(
        hidden.astype(jnp.bfloat16),
        down_ref[...],
        (((1,), (1,)), ((), ())),
        preferred_element_type=jnp.float32,
    )


def fused_kernel(
    n_exp, tok_hbm, ids_ref, logits_ref, gate_hbm, up_hbm, down_hbm, out_ref,
    tok, held, part, core_in, x_in, y_in, x_diag, y_diag, d_chain, o_chain,
    gate_ref, up_ref, down_ref, send_sem, recv_sem, load_sem,
):
    n_z = n_exp // 2
    reach = n_z // 2
    n_rows, width = out_ref.shape
    lanes = held.shape[2]
    rows = held.shape[1]
    batches = n_rows // rows
    half = rows // 2
    spare = width // LANES * LANES
    expert, dp = lax.axis_index("expert"), lax.axis_index("dp")
    z, y = lax.div(expert, 2), lax.rem(expert, 2)
    x, core = lax.div(dp, 2), lax.rem(dp, 2)
    to_x = (expert, (1 - x) * 2 + core)
    to_y = (z * 2 + 1 - y, dp)
    to_core = (expert, x * 2 + 1 - core)
    columns = {"o": y * 2 + x, "x": y * 2 + 1 - x, "y": (1 - y) * 2 + x, "d": (1 - y) * 2 + 1 - x}
    order = "oxyd"

    def to_z(place):
        return (place * 2 + y, dp)

    short = jnp.minimum(z, n_z - 1 - z)
    inward = jnp.where(z * 2 < n_z - 1, 1, -1)

    def near(i):
        if i == 0:
            return z
        paired = z - inward * ((i + 1) // 2) if i % 2 else z + inward * (i // 2)
        return jnp.where(i <= 2 * short, paired, z + inward * (i - short))

    class Plane:
        def __init__(self, i):
            self.i, self.zz = i, near(i)
            self.dist = jnp.abs(self.zz - z)
            self.away = jnp.where(self.zz < z, 1, -1)
            self.out = z + self.away
            self.back = z - self.away
            self.has_out = (self.out >= 0) & (self.out < n_z)
            self.maybe_far = i > reach
            self.far = self.dist > reach
            self.out_d = self.has_out & (self.dist < reach)

    planes = [Plane(i) for i in range(n_z)]
    others = range(1, n_z)

    def block(column, which, zz, h):
        return ((h * 4 + columns[column]) * 2 + which) * n_z + zz

    kinds = {}
    n_recv = [0]

    def recv_index(kind, at):
        if kind not in kinds:
            size = RECV[kind](n_z, batches)
            kinds[kind] = n_recv[0]
            n_recv[0] += size
        return kinds[kind] + at

    for kind in RECV:
        recv_index(kind, 0)

    def at(kind, h, zz):
        return recv_index(kind, h * n_z + zz)

    def at_core(h, column, zz):
        return recv_index("core", (h * 4 + order.index(column)) * n_z + zz)

    def at_chain(kind, h, slot):
        return recv_index(kind, h * (n_z + 1) + slot)

    sent = []

    def when(condition, action):
        if condition is None:
            action()
        else:
            pl.when(condition)(action)

    def start(index, source, target, device, condition=None):
        copy = pltpu.make_async_remote_copy(
            src_ref=source,
            dst_ref=target,
            send_sem=send_sem.at[len(sent)],
            recv_sem=recv_sem.at[index],
            device_id=device,
            device_id_type=pl.DeviceIdType.MESH,
        )
        sent.append((condition, copy))
        when(condition, copy.start)

    def arrived(index, target, condition=None):
        copy = pltpu.make_async_remote_copy(
            src_ref=target,
            dst_ref=target,
            send_sem=send_sem.at[0],
            recv_sem=recv_sem.at[index],
            device_id=to_core,
            device_id_type=pl.DeviceIdType.MESH,
        )
        when(condition, copy.wait_recv)

    tok_load = pltpu.make_async_copy(tok_hbm, tok, load_sem.at[3])
    tok_load.start()
    loads = [
        pltpu.make_async_copy(source, target, load_sem.at[i])
        for i, (source, target) in enumerate(((gate_hbm, gate_ref), (up_hbm, up_ref), (down_hbm, down_ref)))
    ]
    for load in loads:
        load.start()

    above, below = z < n_z - 1, z > 0
    barrier = pltpu.get_barrier_semaphore()

    def greet(device):
        pl.semaphore_signal(barrier, inc=1, device_id=device, device_id_type=pl.DeviceIdType.MESH)

    for device in (to_x, to_y, to_core):
        greet(device)
    pl.when(above)(lambda: greet(to_z(z + 1)))
    pl.when(below)(lambda: greet(to_z(z - 1)))

    wts = jnp.exp(logits_ref[...])
    wts = wts / jnp.sum(wts, axis=0, keepdims=True)
    ids = ids_ref[...]
    by_expert = jnp.concatenate(
        [jnp.sum(jnp.where(ids == e, wts, 0.0), axis=0, keepdims=True) for e in range(n_exp)], axis=0
    )
    high = by_expert.astype(jnp.bfloat16).astype(jnp.float32)
    pairs = jnp.concatenate([high, by_expert - high], axis=0)
    filled = jnp.concatenate(
        [pairs, jnp.zeros((lanes - width - pairs.shape[0], n_rows), jnp.float32)], axis=0
    ).astype(jnp.bfloat16)
    eye = (
        lax.broadcasted_iota(jnp.int32, (n_rows, n_rows), 0)
        == lax.broadcasted_iota(jnp.int32, (n_rows, n_rows), 1)
    ).astype(jnp.float32).astype(jnp.bfloat16)
    extra_cols = lax.dot_general(
        eye, filled, (((1,), (1,)), ((), ())), preferred_element_type=jnp.float32
    ).astype(jnp.bfloat16)
    tok_load.wait()
    for h in range(batches):
        own = block("o", core, z, h)
        held[own, :, :width] = tok[h * rows : (h + 1) * rows]
        held[own, :, width:] = extra_cols[h * rows : (h + 1) * rows]
    pl.semaphore_wait(barrier, 3 + above.astype(jnp.int32) + below.astype(jnp.int32))

    def send_own(h):
        own = held.at[block("o", core, z, h)]
        start(at("x", h, z), own, own, to_x)
        start(at("y", h, z), own, own, to_y)
        start(at("o", h, z), own, own, to_z(z + 1), above)
        start(at("o", h, z), own, own, to_z(z - 1), below)
        start(at_core(h, "o", z), own, own, to_core)

    def take_x(h, i):
        p = planes[i]
        spot = block("x", core, p.zz, h)
        arrived(at("x", h, p.zz), held.at[spot])
        upper = held.at[spot, pl.ds(0, half)]
        if i == 0 or p.maybe_far:
            start(at("y2", h, p.zz), upper, upper, to_y, p.far if i else None)
        start(at_core(h, "x", p.zz), held.at[spot], held.at[spot], to_core)

    def take_y(h, i):
        p = planes[i]
        spot = block("y", core, p.zz, h)
        arrived(at("y", h, p.zz), held.at[spot])
        lower = held.at[spot, pl.ds(half, half)]
        if i == 0 or p.maybe_far:
            start(at("x2", h, p.zz), lower, lower, to_x, p.far if i else None)
        start(at_core(h, "y", p.zz), held.at[spot], held.at[spot], to_core)

    def take_xy(h, i):
        take_x(h, i)
        take_y(h, i)

    def take_o(h, i):
        p = planes[i]
        spot = held.at[block("o", core, p.zz, h)]
        arrived(at("o", h, p.zz), spot)
        start(at("o", h, p.zz), spot, spot, to_z(p.out), p.has_out)
        start(at("x", h, p.zz), spot, spot, to_x)
        start(at("y", h, p.zz), spot, spot, to_y)
        start(at_core(h, "o", p.zz), spot, spot, to_core)

    def take_d(h, i):
        p = planes[i]
        index = block("d", core, p.zz, h)
        spot = held.at[index]

        def halves(condition):
            arrived(at("x2", h, p.zz), held.at[index, pl.ds(half, half)], condition)
            arrived(at("y2", h, p.zz), held.at[index, pl.ds(0, half)], condition)

        if i == 0:
            halves(None)
            start(at("d", h, z), spot, spot, to_z(z + 1), above)
            start(at("d", h, z), spot, spot, to_z(z - 1), below)
        else:
            if p.maybe_far:
                halves(p.far)
            arrived(at("d", h, p.zz), spot, p.dist <= reach if p.maybe_far else None)
            start(at("d", h, p.zz), spot, spot, to_z(p.out), p.out_d)
        start(at_core(h, "d", p.zz), spot, spot, to_core)

    loaded = []

    def product(h, column):
        for zz in range(n_z):
            arrived(at_core(h, column, zz), held.at[block(column, 1 - core, zz, h)])
        if not loaded:
            for load in loads:
                load.wait()
            loaded.append(True)
        span = pl.ds(block(column, 0, 0, h), 2 * n_z)
        rows_in = held[span, :, :width].reshape(2 * n_z * rows, width)
        extra = held[span, :, spare:lanes].reshape(2 * n_z * rows, lanes - spare)
        result = tile_product(n_exp, rows_in, extra, gate_ref, up_ref, down_ref)
        part[span] = result.astype(part.dtype).reshape(2 * n_z, rows, width)
        start(
            recv_index("p", h * 4 + order.index(column)),
            part.at[pl.ds(block(column, 1 - core, 0, h), n_z)],
            core_in.at[pl.ds((h * 4 + order.index(column)) * n_z, n_z)],
            to_core,
        )

    def chained(chain, slot):
        chain[slot] = jnp.zeros(chain.shape[1:], chain.dtype)

    def clear():
        for h in range(batches):
            base = h * (n_z + 1)
            for p in planes[1:]:
                missing = (p.back < 0) | (p.back >= n_z)
                flipped = z + p.away
                no_up = (flipped < 0) | (flipped >= n_z)
                pl.when(no_up)(lambda p=p, base=base: chained(o_chain, base + p.zz))
                pl.when(no_up | (p.dist >= reach))(lambda p=p, base=base: chained(d_chain, base + p.zz))
                if p.maybe_far:

                    @pl.when(jnp.logical_not(p.far))
                    def _(p=p, h=h):
                        chained(x_diag, h * n_z + p.zz)
                        chained(y_diag, h * n_z + p.zz)

            for chain in (o_chain, d_chain):
                pl.when(z == 0)(lambda chain=chain, base=base: chained(chain, base + z))
                pl.when(z == n_z - 1)(lambda chain=chain, base=base: chained(chain, base + n_z))

    step = 16 if half % 16 == 0 else half

    def combined(h, column, zz, *more, target=None):
        spot = block(column, core, zz, h)
        place = (h * 4 + order.index(column)) * n_z + zz

        @pl.loop(0, rows // step)
        def _(k):
            span = pl.ds(k * step, step)
            total = part[spot, span].astype(jnp.float32) + core_in[place, span].astype(jnp.float32)
            for source, index in more:
                total = total + source[index, span].astype(jnp.float32)
            if target is None:
                part[spot, span] = total.astype(part.dtype)
            else:
                out_ref[pl.ds(target + k * step, step)] = total.astype(out_ref.dtype)

        return spot

    seen = set()

    def need(h, column):
        if (h, column) not in seen:
            seen.add((h, column))
            base = (h * 4 + order.index(column)) * n_z
            arrived(recv_index("p", h * 4 + order.index(column)), core_in.at[pl.ds(base, n_z)])

    def slot_at(p):
        toward = z - p.away
        return jnp.where((toward == p.zz) & (p.away > 0), n_z, p.zz)

    def give_d(h, i):
        p = planes[i]
        base = h * (n_z + 1)
        need(h, "d")
        if i == 0:
            arrived(at_chain("dc", h, z), d_chain.at[base + z], below)
            arrived(at_chain("dc", h, n_z), d_chain.at[base + n_z], above)
            spot = combined(h, "d", z, (d_chain, base + z), (d_chain, base + n_z))
        else:
            has_up = p.has_out & (p.dist < reach)
            arrived(at_chain("dc", h, p.zz), d_chain.at[base + p.zz], has_up)
            spot = combined(h, "d", p.zz, (d_chain, base + p.zz))
            start(
                at_chain("dc", h, slot_at(p)), part.at[spot], d_chain.at[base + slot_at(p)], to_z(p.back),
                jnp.logical_not(p.far) if p.maybe_far else None,
            )
        if i == 0 or p.maybe_far:
            condition = p.far if i else None
            start(at("dx", h, p.zz), part.at[spot, pl.ds(half, half)], x_diag.at[h * n_z + p.zz], to_x, condition)
            start(at("dy", h, p.zz), part.at[spot, pl.ds(0, half)], y_diag.at[h * n_z + p.zz], to_y, condition)

    def give_x(h, i):
        p = planes[i]
        need(h, "x")
        index = h * n_z + p.zz
        spot = combined(h, "x", p.zz)
        if i == 0 or p.maybe_far:
            arrived(at("dy", h, p.zz), y_diag.at[index], p.far if i else None)
            part[spot, :half] = (
                part[spot, :half].astype(jnp.float32) + y_diag[index].astype(jnp.float32)
            ).astype(part.dtype)
        start(at("rx", h, p.zz), part.at[spot], x_in.at[index], to_x)

    def give_y(h, i):
        p = planes[i]
        need(h, "y")
        index = h * n_z + p.zz
        spot = combined(h, "y", p.zz)
        if i == 0 or p.maybe_far:
            arrived(at("dx", h, p.zz), x_diag.at[index], p.far if i else None)
            part[spot, half:] = (
                part[spot, half:].astype(jnp.float32) + x_diag[index].astype(jnp.float32)
            ).astype(part.dtype)
        start(at("ry", h, p.zz), part.at[spot], y_in.at[index], to_y)

    def give_xy(h, i):
        give_x(h, i)
        give_y(h, i)

    def give_o(h, i):
        p = planes[i]
        base = h * (n_z + 1)
        index = h * n_z + p.zz
        need(h, "o")
        arrived(at("rx", h, p.zz), x_in.at[index])
        arrived(at("ry", h, p.zz), y_in.at[index])
        if i == 0:
            arrived(at_chain("oc", h, z), o_chain.at[base + z], below)
            arrived(at_chain("oc", h, n_z), o_chain.at[base + n_z], above)
            combined(
                h, "o", z, (x_in, index), (y_in, index), (o_chain, base + z), (o_chain, base + n_z),
                target=h * rows,
            )
        else:
            arrived(at_chain("oc", h, p.zz), o_chain.at[base + p.zz], p.has_out)
            spot = combined(h, "o", p.zz, (x_in, index), (y_in, index), (o_chain, base + p.zz))
            start(at_chain("oc", h, slot_at(p)), part.at[spot], o_chain.at[base + slot_at(p)], to_z(p.back))

    steps = {
        "own": send_own, "clear": clear, "x": take_x, "y": take_y, "xy": take_xy, "o": take_o, "d": take_d,
        "C": product, "Rd": give_d, "Rx": give_x, "Ry": give_y, "Rxy": give_xy, "Ro": give_o,
    }
    for name, *numbers in PLAN:
        steps[name](*numbers)
    for condition, copy in sent:
        when(condition, copy.wait_send)


RECV = {kind: (lambda n_z, batches: n_z * batches) for kind in ("x", "y", "o", "d", "x2", "y2", "dx", "dy", "rx", "ry")}
RECV["core"] = lambda n_z, batches: 4 * n_z * batches
RECV["p"] = lambda n_z, batches: 4 * batches
RECV["dc"] = RECV["oc"] = lambda n_z, batches: (n_z + 1) * batches


PLAN = (
    ("own", 0),
    ("own", 1),
    ("x", 0, 0),
    ("clear",),
    ("y", 0, 0),
    ("o", 0, 1),
    ("o", 0, 2),
    ("x", 1, 0),
    ("y", 1, 0),
    ("d", 0, 0),
    ("o", 0, 3),
    ("o", 1, 1),
    ("x", 0, 2),
    ("x", 0, 1),
    ("y", 0, 1),
    ("d", 0, 2),
    ("d", 0, 1),
    ("C", 0, "o"),
    ("x", 0, 3),
    ("y", 0, 3),
    ("o", 1, 3),
    ("d", 0, 3),
    ("C", 0, "x"),
    ("o", 1, 2),
    ("d", 1, 0),
    ("y", 0, 2),
    ("y", 1, 1),
    ("C", 0, "d"),
    ("x", 1, 3),
    ("x", 1, 1),
    ("y", 1, 3),
    ("C", 0, "y"),
    ("Rx", 0, 2),
    ("Rd", 0, 3),
    ("x", 1, 2),
    ("d", 1, 2),
    ("d", 1, 1),
    ("Rd", 0, 2),
    ("d", 1, 3),
    ("Ry", 0, 1),
    ("y", 1, 2),
    ("Rx", 0, 1),
    ("Rd", 0, 1),
    ("Ry", 0, 2),
    ("C", 1, "d"),
    ("C", 1, "x"),
    ("Rd", 1, 3),
    ("Ry", 0, 3),
    ("Rd", 1, 2),
    ("Rx", 0, 3),
    ("C", 1, "y"),
    ("Ro", 0, 2),
    ("Rd", 0, 0),
    ("Rx", 1, 3),
    ("Rx", 1, 2),
    ("Rd", 1, 1),
    ("Ry", 1, 3),
    ("Rx", 1, 1),
    ("Ry", 1, 2),
    ("Ro", 0, 3),
    ("Ry", 1, 1),
    ("C", 1, "o"),
    ("Ro", 1, 3),
    ("Rd", 1, 0),
    ("Ry", 0, 0),
    ("Rx", 0, 0),
    ("Ro", 1, 2),
    ("Ro", 0, 1),
    ("Rx", 1, 0),
    ("Ro", 1, 1),
    ("Ry", 1, 0),
    ("Ro", 0, 0),
    ("Ro", 1, 0),
)


def fused_device(tokens, expert_ids, gate_logits, w_gate, w_up, w_down):
    n_rows, width = tokens.shape
    hidden_width = w_gate.shape[2]
    n_exp = lax.axis_size("expert")
    n_z = n_exp // 2
    batches = 2
    rows = n_rows // batches
    lanes = round_up(width + 2 * n_exp, LANES)
    total = n_exp * lax.axis_size("dp") * batches
    receives = sum(size(n_z, batches) for size in RECV.values())
    sends = 64 * n_z
    bf16 = jnp.bfloat16
    in_vmem = pl.BlockSpec(memory_space=pltpu.VMEM)
    anywhere = pl.BlockSpec(memory_space=pl.ANY)
    return pl.pallas_call(
        functools.partial(fused_kernel, n_exp),
        in_specs=[anywhere, in_vmem, in_vmem, anywhere, anywhere, anywhere],
        out_specs=in_vmem,
        out_shape=jax.ShapeDtypeStruct((n_rows, width), bf16),
        scratch_shapes=[
            pltpu.VMEM((n_rows, width), bf16),
            pltpu.VMEM((total, rows, lanes), bf16),
            pltpu.VMEM((total, rows, width), bf16),
            pltpu.VMEM((total // 2, rows, width), bf16),
            pltpu.VMEM((batches * n_z, rows, width), bf16),
            pltpu.VMEM((batches * n_z, rows, width), bf16),
            pltpu.VMEM((batches * n_z, rows // 2, width), bf16),
            pltpu.VMEM((batches * n_z, rows // 2, width), bf16),
            pltpu.VMEM((batches * (n_z + 1), rows, width), bf16),
            pltpu.VMEM((batches * (n_z + 1), rows, width), bf16),
            pltpu.VMEM((width, hidden_width), bf16),
            pltpu.VMEM((width, hidden_width), bf16),
            pltpu.VMEM((width, hidden_width), bf16),
            pltpu.SemaphoreType.DMA((sends,)),
            pltpu.SemaphoreType.DMA((receives,)),
            pltpu.SemaphoreType.DMA((4,)),
        ],
        compiler_params=pltpu.CompilerParams(
            collective_id=0, has_side_effects=True, vmem_limit_bytes=64 * 1024 * 1024 - 65536
        ),
    )(tokens, expert_ids.T, gate_logits.T, w_gate[0], w_up[0], w_down[0].T)


def solution(mesh):
    def per_device(tokens, expert_ids, *others):
        n_exp = lax.axis_size("expert")
        if n_exp > 4 * expert_ids.shape[1]:
            return sparse_device(tokens, expert_ids, *others)
        paired = lax.axis_size("dp") == 4 and n_exp % 2 == 0 and tokens.shape[0] % 32 == 0
        return (fused_device if paired else dense_device)(tokens, expert_ids, *others)

    return jax.shard_map(
        per_device,
        mesh=mesh,
        in_specs=(
            P(("expert", "dp"), None),
            P(("expert", "dp"), None),
            P(("expert", "dp"), None),
            P("expert", None, "dp"),
            P("expert", None, "dp"),
            P("expert", "dp", None),
        ),
        out_specs=P(("expert", "dp"), None),
        check_vma=False,
    )
```

```python
import functools

import jax
import jax.numpy as jnp
from jax import lax
from jax.experimental import pallas as pl
from jax.experimental.pallas import tpu as pltpu
from jax.sharding import PartitionSpec as P


def expert_rows(tile_in, gate_w, up_w, down_w):
    gate_val = jnp.dot(tile_in, gate_w, preferred_element_type=jnp.float32)
    up_val = jnp.dot(tile_in, up_w, preferred_element_type=jnp.float32)
    hidden = ((up_val + 1.0) * gate_val * jax.nn.sigmoid(1.702 * gate_val)).astype(jnp.bfloat16)
    return jnp.dot(hidden, down_w, preferred_element_type=jnp.float32).astype(jnp.bfloat16)


def run_tiles(packed, first_row, last_row, gate_w, up_w, down_w):
    tile_rows = 128
    n_tiles = jnp.maximum(last_row - first_row + tile_rows - 1, 0) // tile_rows
    result_buf = jnp.zeros((packed.shape[0], down_w.shape[1]), jnp.bfloat16)

    def advance(index_t, buffer):
        at_row = first_row + index_t * tile_rows
        tile_in = lax.dynamic_slice_in_dim(packed, at_row, tile_rows, 0)
        return lax.dynamic_update_slice_in_dim(
            buffer, expert_rows(tile_in, gate_w, up_w, down_w), at_row, 0
        )

    return lax.fori_loop(0, n_tiles, advance, result_buf)


def sparse_device(tokens, expert_ids, gate_logits, w_gate, w_up, w_down):
    n_rows, width = tokens.shape
    n_tops = expert_ids.shape[1]
    n_exp = lax.axis_size("expert")
    n_dp = lax.axis_size("dp")
    slot_cap = max(2, 3 * n_rows * n_tops // (2 * n_exp))
    tile_rows = 128
    flat_ids = expert_ids.reshape(-1)
    onehot = (flat_ids[:, None] == jnp.arange(n_exp, dtype=jnp.int32)[None, :]).astype(jnp.int32)
    rank_in = jnp.sum((jnp.cumsum(onehot, axis=0) - onehot) * onehot, axis=1)
    counts = jnp.sum(onehot, axis=0)
    slot_idx = flat_ids * slot_cap + rank_in
    source = (
        jnp.zeros((n_exp * slot_cap,), jnp.int32)
        .at[slot_idx]
        .set(jnp.arange(n_rows * n_tops, dtype=jnp.int32) // n_tops)
    )
    filled = (jnp.arange(slot_cap)[None, :] < counts[:, None]).reshape(-1)
    outgoing = jnp.where(filled[:, None], tokens[source], jnp.zeros_like(tokens[source])).reshape(
        n_exp, slot_cap, width
    )
    rows_mid, counts_mid = (
        lax.all_to_all(outgoing, "expert", split_axis=0, concat_axis=0, tiled=True),
        lax.all_to_all(counts[:, None], "expert", split_axis=0, concat_axis=0, tiled=True),
    )
    rows_in, counts_in = (
        lax.all_gather(rows_mid, "dp", axis=0, tiled=True),
        lax.all_gather(counts_mid, "dp", axis=0, tiled=True),
    )
    rows_flat = rows_in.reshape(-1, width)
    total_rows = rows_flat.shape[0]
    live_row = (jnp.arange(slot_cap)[None, :] < counts_in.reshape(-1)[:, None]).reshape(-1)
    position = jnp.cumsum(live_row.astype(jnp.int32)) - 1
    live_total = jnp.sum(live_row.astype(jnp.int32))
    padded = (total_rows + tile_rows - 1) // tile_rows * tile_rows + tile_rows
    gather_idx = (
        jnp.zeros((padded,), jnp.int32)
        .at[jnp.where(live_row, position, padded)]
        .set(jnp.arange(total_rows, dtype=jnp.int32), mode="drop")
    )
    packed = rows_flat[gather_idx]
    gate_w = w_gate[0]
    up_w = w_up[0]
    down_w = w_down[0]
    merged = run_tiles(packed, 0, live_total, gate_w, up_w, down_w)
    slot_out = jnp.where(
        live_row[:, None],
        merged[jnp.where(live_row, position, 0)],
        jnp.zeros((total_rows, width), jnp.bfloat16),
    )
    summed = lax.psum_scatter(
        slot_out.reshape(n_dp * n_exp, slot_cap, width), "dp", scatter_dimension=0, tiled=True
    ).astype(jnp.float32)
    expert_out = lax.all_to_all(
        summed.astype(jnp.bfloat16), "expert", split_axis=0, concat_axis=0, tiled=True
    )
    picked = expert_out.reshape(n_exp * slot_cap, width)[slot_idx]
    gate_wts = jnp.exp(gate_logits)
    gate_wts = gate_wts / jnp.sum(gate_wts, axis=1, keepdims=True)
    mixed = jnp.sum(
        picked.reshape(n_rows, n_tops, width).astype(jnp.float32) * gate_wts[:, :, None], axis=1
    )
    return mixed.astype(jnp.bfloat16)


LANES = 128
CHUNKS = 1


def round_up(value, step):
    return (value + step - 1) // step * step


def routing_columns(expert_ids, gate_logits, n_exp, lanes):
    gate_wts = jnp.exp(gate_logits)
    gate_wts = gate_wts / jnp.sum(gate_wts, axis=1, keepdims=True)
    chosen = expert_ids[:, :, None] == jnp.arange(n_exp, dtype=jnp.int32)[None, None, :]
    by_expert = jnp.sum(jnp.where(chosen, gate_wts[:, :, None], 0.0), axis=1)
    high = by_expert.astype(jnp.bfloat16)
    low = (by_expert - high.astype(jnp.float32)).astype(jnp.bfloat16)
    columns = jnp.concatenate([high, low], axis=1)
    return jnp.pad(columns, ((0, 0), (0, lanes - columns.shape[1])))


def dense_kernel(n_exp, rows_ref, gate_ref, up_ref, down_ref, out_ref):
    width, hidden_width = gate_ref.shape
    lanes = rows_ref.shape[1]
    mine = lax.axis_index("expert")
    rows_in = rows_ref[:, :width]
    gate_val = jnp.dot(rows_in, gate_ref[...], preferred_element_type=jnp.float32)
    up_val = jnp.dot(rows_in, up_ref[...], preferred_element_type=jnp.float32)
    first = width // LANES * LANES
    extra = rows_ref[:, first:lanes].astype(jnp.float32)
    lane = lax.broadcasted_iota(jnp.int32, extra.shape, 1) + first - width
    weight = jnp.sum(jnp.where((lane == mine) | (lane == mine + n_exp), extra, 0.0), axis=1, keepdims=True)
    hidden = (up_val + 1.0) * gate_val * (weight / (1.0 + jnp.exp(-1.702 * gate_val)))
    out_ref[...] = jnp.dot(
        hidden.astype(jnp.bfloat16), down_ref[...], preferred_element_type=jnp.float32
    ).astype(out_ref.dtype)


def dense_rows(rows, gate_w, up_w, down_w, n_exp):
    n_rows, lanes = rows.shape
    width, hidden_width = gate_w.shape
    tile_rows = 256
    while n_rows % tile_rows:
        tile_rows //= 2
    whole = pl.BlockSpec(memory_space=pltpu.VMEM)
    return pl.pallas_call(
        functools.partial(dense_kernel, n_exp),
        grid=(n_rows // tile_rows,),
        in_specs=[pl.BlockSpec((tile_rows, lanes), lambda i: (i, 0)), whole, whole, whole],
        out_specs=pl.BlockSpec((tile_rows, width), lambda i: (i, 0)),
        out_shape=jax.ShapeDtypeStruct((n_rows, width), jnp.bfloat16),
        cost_estimate=pl.CostEstimate(
            flops=6 * n_rows * width * hidden_width,
            bytes_accessed=2 * n_rows * (lanes + width) + 6 * width * hidden_width,
            transcendentals=n_rows * hidden_width,
        ),
    )(rows, gate_w, up_w, down_w)


def dense_device(tokens, expert_ids, gate_logits, w_gate, w_up, w_down):
    n_rows, width = tokens.shape
    n_exp = lax.axis_size("expert")
    both = ("expert", "dp")
    lanes = round_up(width + 2 * n_exp, LANES)
    extra = routing_columns(expert_ids, gate_logits, n_exp, lanes - width)
    wide = jnp.concatenate([tokens, extra], axis=1)
    step = n_rows // CHUNKS
    done = []
    for chunk in range(CHUNKS):
        rows = lax.all_gather(wide[chunk * step : (chunk + 1) * step], both, axis=0, tiled=True)
        partial = dense_rows(rows, w_gate[0], w_up[0], w_down[0], n_exp)
        done.append(lax.psum_scatter(partial, both, scatter_dimension=0, tiled=True))
    return done[0] if CHUNKS == 1 else jnp.concatenate(done, axis=0)


def tile_product(n_exp, rows_in, extra, gate_ref, up_ref, down_ref):
    width = gate_ref.shape[0]
    mine = lax.axis_index("expert")
    gate_val = jnp.dot(rows_in, gate_ref[...], preferred_element_type=jnp.float32)
    up_val = jnp.dot(rows_in, up_ref[...], preferred_element_type=jnp.float32)
    extra = extra.astype(jnp.float32)
    lane = lax.broadcasted_iota(jnp.int32, extra.shape, 1) - width % LANES
    weight = jnp.sum(jnp.where((lane == mine) | (lane == mine + n_exp), extra, 0.0), axis=1, keepdims=True)
    hidden = (up_val + 1.0) * gate_val * (weight / (1.0 + jnp.exp(-1.702 * gate_val)))
    return lax.dot_general(
        hidden.astype(jnp.bfloat16),
        down_ref[...],
        (((1,), (1,)), ((), ())),
        preferred_element_type=jnp.float32,
    )


def fused_kernel(
    n_exp, tok_hbm, ids_hbm, logits_hbm, gate_hbm, up_hbm, down_hbm, out_ref,
    ids_ref, logits_ref, tok, held, part, core_in, x_in, y_in, x_diag, y_diag, d_chain, o_chain,
    gate_ref, up_ref, down_ref, send_sem, recv_sem, load_sem,
):
    n_z = n_exp // 2
    reach = n_z // 2
    n_rows, width = out_ref.shape
    lanes = held.shape[2]
    rows = held.shape[1]
    batches = n_rows // rows
    half = rows // 2
    spare = width // LANES * LANES
    expert, dp = lax.axis_index("expert"), lax.axis_index("dp")
    z, y = lax.div(expert, 2), lax.rem(expert, 2)
    x, core = lax.div(dp, 2), lax.rem(dp, 2)
    to_x = (expert, (1 - x) * 2 + core)
    to_y = (z * 2 + 1 - y, dp)
    to_core = (expert, x * 2 + 1 - core)
    columns = {"o": y * 2 + x, "x": y * 2 + 1 - x, "y": (1 - y) * 2 + x, "d": (1 - y) * 2 + 1 - x}
    order = "oxyd"

    def to_z(place):
        return (place * 2 + y, dp)

    short = jnp.minimum(z, n_z - 1 - z)
    inward = jnp.where(z * 2 < n_z - 1, 1, -1)

    def near(i):
        if i == 0:
            return z
        paired = z - inward * ((i + 1) // 2) if i % 2 else z + inward * (i // 2)
        return jnp.where(i <= 2 * short, paired, z + inward * (i - short))

    class Plane:
        def __init__(self, i):
            self.i, self.zz = i, near(i)
            self.dist = jnp.abs(self.zz - z)
            self.away = jnp.where(self.zz < z, 1, -1)
            self.out = z + self.away
            self.back = z - self.away
            self.has_out = (self.out >= 0) & (self.out < n_z)
            self.maybe_far = i > reach
            self.far = self.dist > reach
            self.out_d = self.has_out & (self.dist < reach)

    planes = [Plane(i) for i in range(n_z)]
    others = range(1, n_z)

    def block(column, which, zz, h):
        return ((h * 4 + columns[column]) * 2 + which) * n_z + zz

    kinds = {}
    n_recv = [0]

    def recv_index(kind, at):
        if kind not in kinds:
            size = RECV[kind](n_z, batches)
            kinds[kind] = n_recv[0]
            n_recv[0] += size
        return kinds[kind] + at

    for kind in RECV:
        recv_index(kind, 0)

    def at(kind, h, zz):
        return recv_index(kind, h * n_z + zz)

    def at_core(h, column, zz):
        return recv_index("core", (h * 4 + order.index(column)) * n_z + zz)

    def at_chain(kind, h, slot):
        return recv_index(kind, h * (n_z + 1) + slot)

    sent = []

    def when(condition, action):
        if condition is None:
            action()
        else:
            pl.when(condition)(action)

    def start(index, source, target, device, condition=None):
        copy = pltpu.make_async_remote_copy(
            src_ref=source,
            dst_ref=target,
            send_sem=send_sem.at[len(sent)],
            recv_sem=recv_sem.at[index],
            device_id=device,
            device_id_type=pl.DeviceIdType.MESH,
        )
        sent.append((condition, copy))
        when(condition, copy.start)

    def arrived(index, target, condition=None):
        copy = pltpu.make_async_remote_copy(
            src_ref=target,
            dst_ref=target,
            send_sem=send_sem.at[0],
            recv_sem=recv_sem.at[index],
            device_id=to_core,
            device_id_type=pl.DeviceIdType.MESH,
        )
        when(condition, copy.wait_recv)

    above, below = z < n_z - 1, z > 0
    barrier = pltpu.get_barrier_semaphore()

    def greet(device):
        pl.semaphore_signal(barrier, inc=1, device_id=device, device_id_type=pl.DeviceIdType.MESH)

    for device in (to_x, to_y, to_core):
        greet(device)
    pl.when(above)(lambda: greet(to_z(z + 1)))
    pl.when(below)(lambda: greet(to_z(z - 1)))

    small = [
        pltpu.make_async_copy(source, target, load_sem.at[i])
        for i, (source, target) in enumerate(((ids_hbm, ids_ref), (logits_hbm, logits_ref), (tok_hbm, tok)))
    ]
    for load in small:
        load.start()
    loads = [
        pltpu.make_async_copy(source, target, load_sem.at[3 + i])
        for i, (source, target) in enumerate(((gate_hbm, gate_ref), (up_hbm, up_ref), (down_hbm, down_ref)))
    ]
    small[0].wait()
    small[1].wait()
    wts = jnp.exp(logits_ref[...])
    wts = wts / jnp.sum(wts, axis=0, keepdims=True)
    ids = ids_ref[...]
    by_expert = jnp.concatenate(
        [jnp.sum(jnp.where(ids == e, wts, 0.0), axis=0, keepdims=True) for e in range(n_exp)], axis=0
    )
    high = by_expert.astype(jnp.bfloat16).astype(jnp.float32)
    pairs = jnp.concatenate([high, by_expert - high], axis=0)
    filled = jnp.concatenate(
        [pairs, jnp.zeros((lanes - width - pairs.shape[0], n_rows), jnp.float32)], axis=0
    ).astype(jnp.bfloat16)
    eye = (
        lax.broadcasted_iota(jnp.int32, (n_rows, n_rows), 0)
        == lax.broadcasted_iota(jnp.int32, (n_rows, n_rows), 1)
    ).astype(jnp.float32).astype(jnp.bfloat16)
    extra_cols = lax.dot_general(
        eye, filled, (((1,), (1,)), ((), ())), preferred_element_type=jnp.float32
    ).astype(jnp.bfloat16)
    small[2].wait()
    for load in loads:
        load.start()
    for h in range(batches):
        own = block("o", core, z, h)
        held[own, :, :width] = tok[h * rows : (h + 1) * rows]
        held[own, :, width:] = extra_cols[h * rows : (h + 1) * rows]
    pl.semaphore_wait(barrier, 3 + above.astype(jnp.int32) + below.astype(jnp.int32))

    def send_own(h):
        own = held.at[block("o", core, z, h)]
        start(at("x", h, z), own, own, to_x)
        start(at("y", h, z), own, own, to_y)
        start(at("o", h, z), own, own, to_z(z + 1), above)
        start(at("o", h, z), own, own, to_z(z - 1), below)
        start(at_core(h, "o", z), own, own, to_core)

    def take_x(h, i):
        p = planes[i]
        spot = block("x", core, p.zz, h)
        arrived(at("x", h, p.zz), held.at[spot])
        upper = held.at[spot, pl.ds(0, half)]
        if i == 0 or p.maybe_far:
            start(at("y2", h, p.zz), upper, upper, to_y, p.far if i else None)
        start(at_core(h, "x", p.zz), held.at[spot], held.at[spot], to_core)

    def take_y(h, i):
        p = planes[i]
        spot = block("y", core, p.zz, h)
        arrived(at("y", h, p.zz), held.at[spot])
        lower = held.at[spot, pl.ds(half, half)]
        if i == 0 or p.maybe_far:
            start(at("x2", h, p.zz), lower, lower, to_x, p.far if i else None)
        start(at_core(h, "y", p.zz), held.at[spot], held.at[spot], to_core)

    def take_xy(h, i):
        take_x(h, i)
        take_y(h, i)

    def take_o(h, i):
        p = planes[i]
        spot = held.at[block("o", core, p.zz, h)]
        arrived(at("o", h, p.zz), spot)
        start(at("o", h, p.zz), spot, spot, to_z(p.out), p.has_out)
        start(at("x", h, p.zz), spot, spot, to_x)
        start(at("y", h, p.zz), spot, spot, to_y)
        start(at_core(h, "o", p.zz), spot, spot, to_core)

    def take_d(h, i):
        p = planes[i]
        index = block("d", core, p.zz, h)
        spot = held.at[index]

        def halves(condition):
            arrived(at("x2", h, p.zz), held.at[index, pl.ds(half, half)], condition)
            arrived(at("y2", h, p.zz), held.at[index, pl.ds(0, half)], condition)

        if i == 0:
            halves(None)
            start(at("d", h, z), spot, spot, to_z(z + 1), above)
            start(at("d", h, z), spot, spot, to_z(z - 1), below)
        else:
            if p.maybe_far:
                halves(p.far)
            arrived(at("d", h, p.zz), spot, p.dist <= reach if p.maybe_far else None)
            start(at("d", h, p.zz), spot, spot, to_z(p.out), p.out_d)
        start(at_core(h, "d", p.zz), spot, spot, to_core)

    loaded = []

    def product(h, column):
        for zz in range(n_z):
            arrived(at_core(h, column, zz), held.at[block(column, 1 - core, zz, h)])
        if not loaded:
            for load in loads:
                load.wait()
            loaded.append(True)
        span = pl.ds(block(column, 0, 0, h), 2 * n_z)
        rows_in = held[span, :, :width].reshape(2 * n_z * rows, width)
        extra = held[span, :, spare:lanes].reshape(2 * n_z * rows, lanes - spare)
        result = tile_product(n_exp, rows_in, extra, gate_ref, up_ref, down_ref)
        part[span] = result.astype(part.dtype).reshape(2 * n_z, rows, width)
        start(
            recv_index("p", h * 4 + order.index(column)),
            part.at[pl.ds(block(column, 1 - core, 0, h), n_z)],
            core_in.at[pl.ds((h * 4 + order.index(column)) * n_z, n_z)],
            to_core,
        )

    def chained(chain, slot):
        chain[slot] = jnp.zeros(chain.shape[1:], chain.dtype)

    def clear():
        for h in range(batches):
            base = h * (n_z + 1)
            for p in planes[1:]:
                missing = (p.back < 0) | (p.back >= n_z)
                flipped = z + p.away
                no_up = (flipped < 0) | (flipped >= n_z)
                pl.when(no_up)(lambda p=p, base=base: chained(o_chain, base + p.zz))
                pl.when(no_up | (p.dist >= reach))(lambda p=p, base=base: chained(d_chain, base + p.zz))
                if p.maybe_far:

                    @pl.when(jnp.logical_not(p.far))
                    def _(p=p, h=h):
                        chained(x_diag, h * n_z + p.zz)
                        chained(y_diag, h * n_z + p.zz)

            for chain in (o_chain, d_chain):
                pl.when(z == 0)(lambda chain=chain, base=base: chained(chain, base + z))
                pl.when(z == n_z - 1)(lambda chain=chain, base=base: chained(chain, base + n_z))

    step = 16 if rows % 16 == 0 else rows

    def combined(h, column, zz, *more, target=None):
        spot = block(column, core, zz, h)
        place = (h * 4 + order.index(column)) * n_z + zz

        @pl.loop(0, rows // step)
        def _(k):
            span = pl.ds(k * step, step)
            total = part[spot, span].astype(jnp.float32) + core_in[place, span].astype(jnp.float32)
            for source, index in more:
                total = total + source[index, span].astype(jnp.float32)
            if target is None:
                part[spot, span] = total.astype(part.dtype)
            else:
                out_ref[pl.ds(target + k * step, step)] = total.astype(out_ref.dtype)

        return spot

    seen = set()

    def need(h, column):
        if (h, column) not in seen:
            seen.add((h, column))
            base = (h * 4 + order.index(column)) * n_z
            arrived(recv_index("p", h * 4 + order.index(column)), core_in.at[pl.ds(base, n_z)])

    def slot_at(p):
        toward = z - p.away
        return jnp.where((toward == p.zz) & (p.away > 0), n_z, p.zz)

    def give_d(h, i):
        p = planes[i]
        base = h * (n_z + 1)
        need(h, "d")
        if i == 0:
            arrived(at_chain("dc", h, z), d_chain.at[base + z], below)
            arrived(at_chain("dc", h, n_z), d_chain.at[base + n_z], above)
            spot = combined(h, "d", z, (d_chain, base + z), (d_chain, base + n_z))
        else:
            has_up = p.has_out & (p.dist < reach)
            arrived(at_chain("dc", h, p.zz), d_chain.at[base + p.zz], has_up)
            spot = combined(h, "d", p.zz, (d_chain, base + p.zz))
            start(
                at_chain("dc", h, slot_at(p)), part.at[spot], d_chain.at[base + slot_at(p)], to_z(p.back),
                jnp.logical_not(p.far) if p.maybe_far else None,
            )
        if i == 0 or p.maybe_far:
            condition = p.far if i else None
            start(at("dx", h, p.zz), part.at[spot, pl.ds(half, half)], x_diag.at[h * n_z + p.zz], to_x, condition)
            start(at("dy", h, p.zz), part.at[spot, pl.ds(0, half)], y_diag.at[h * n_z + p.zz], to_y, condition)

    def give_x(h, i):
        p = planes[i]
        need(h, "x")
        index = h * n_z + p.zz
        spot = combined(h, "x", p.zz)
        if i == 0 or p.maybe_far:
            arrived(at("dy", h, p.zz), y_diag.at[index], p.far if i else None)
            part[spot, :half] = (
                part[spot, :half].astype(jnp.float32) + y_diag[index].astype(jnp.float32)
            ).astype(part.dtype)
        start(at("rx", h, p.zz), part.at[spot], x_in.at[index], to_x)

    def give_y(h, i):
        p = planes[i]
        need(h, "y")
        index = h * n_z + p.zz
        spot = combined(h, "y", p.zz)
        if i == 0 or p.maybe_far:
            arrived(at("dx", h, p.zz), x_diag.at[index], p.far if i else None)
            part[spot, half:] = (
                part[spot, half:].astype(jnp.float32) + x_diag[index].astype(jnp.float32)
            ).astype(part.dtype)
        start(at("ry", h, p.zz), part.at[spot], y_in.at[index], to_y)

    def give_xy(h, i):
        give_x(h, i)
        give_y(h, i)

    def give_o(h, i):
        p = planes[i]
        base = h * (n_z + 1)
        index = h * n_z + p.zz
        need(h, "o")
        arrived(at("rx", h, p.zz), x_in.at[index])
        arrived(at("ry", h, p.zz), y_in.at[index])
        if i == 0:
            arrived(at_chain("oc", h, z), o_chain.at[base + z], below)
            arrived(at_chain("oc", h, n_z), o_chain.at[base + n_z], above)
            combined(
                h, "o", z, (x_in, index), (y_in, index), (o_chain, base + z), (o_chain, base + n_z),
                target=h * rows,
            )
        else:
            arrived(at_chain("oc", h, p.zz), o_chain.at[base + p.zz], p.has_out)
            spot = combined(h, "o", p.zz, (x_in, index), (y_in, index), (o_chain, base + p.zz))
            start(at_chain("oc", h, slot_at(p)), part.at[spot], o_chain.at[base + slot_at(p)], to_z(p.back))

    steps = {
        "own": send_own, "clear": clear, "x": take_x, "y": take_y, "xy": take_xy, "o": take_o, "d": take_d,
        "C": product, "Rd": give_d, "Rx": give_x, "Ry": give_y, "Rxy": give_xy, "Ro": give_o,
    }
    for name, *numbers in PLAN:
        steps[name](*numbers)
    for condition, copy in sent:
        when(condition, copy.wait_send)


RECV = {kind: (lambda n_z, batches: n_z * batches) for kind in ("x", "y", "o", "d", "x2", "y2", "dx", "dy", "rx", "ry")}
RECV["core"] = lambda n_z, batches: 4 * n_z * batches
RECV["p"] = lambda n_z, batches: 4 * batches
RECV["dc"] = RECV["oc"] = lambda n_z, batches: (n_z + 1) * batches


BATCHES = 2

PLAN = (
    ("own", 0),
    ("clear",),
    ("own", 1),
    ("x", 0, 0),
    ("y", 0, 0),
    ("o", 0, 1),
    ("o", 0, 2),
    ("x", 1, 0),
    ("y", 1, 0),
    ("d", 0, 0),
    ("o", 0, 3),
    ("y", 0, 1),
    ("o", 1, 1),
    ("x", 0, 1),
    ("C", 0, "o"),
    ("y", 0, 2),
    ("d", 0, 1),
    ("d", 0, 2),
    ("x", 0, 2),
    ("y", 0, 3),
    ("x", 0, 3),
    ("o", 1, 3),
    ("d", 0, 3),
    ("C", 0, "y"),
    ("o", 1, 2),
    ("d", 1, 0),
    ("y", 1, 1),
    ("C", 0, "d"),
    ("y", 1, 3),
    ("x", 1, 3),
    ("C", 0, "x"),
    ("Rd", 0, 3),
    ("Ry", 0, 2),
    ("Ry", 0, 1),
    ("d", 1, 2),
    ("d", 1, 1),
    ("Rd", 0, 2),
    ("d", 1, 3),
    ("Rx", 0, 1),
    ("Rd", 0, 1),
    ("x", 1, 2),
    ("y", 1, 2),
    ("Rx", 0, 2),
    ("x", 1, 1),
    ("C", 1, "d"),
    ("Rx", 0, 3),
    ("C", 1, "x"),
    ("Rd", 1, 3),
    ("Rd", 1, 2),
    ("Ry", 0, 3),
    ("C", 1, "y"),
    ("Ro", 0, 2),
    ("Rd", 0, 0),
    ("Rx", 1, 3),
    ("Rx", 1, 2),
    ("Rx", 1, 1),
    ("Rd", 1, 1),
    ("Ry", 1, 3),
    ("Ry", 1, 2),
    ("Ry", 1, 1),
    ("C", 1, "o"),
    ("Ro", 0, 3),
    ("Ro", 1, 3),
    ("Rd", 1, 0),
    ("Rx", 0, 0),
    ("Ry", 0, 0),
    ("Ro", 1, 2),
    ("Ro", 0, 1),
    ("Ro", 1, 1),
    ("Rx", 1, 0),
    ("Ry", 1, 0),
    ("Ro", 0, 0),
    ("Ro", 1, 0),
)


def fused_device(tokens, expert_ids, gate_logits, w_gate, w_up, w_down):
    n_rows, width = tokens.shape
    hidden_width = w_gate.shape[2]
    n_exp = lax.axis_size("expert")
    n_z = n_exp // 2
    batches = BATCHES
    rows = n_rows // batches
    lanes = round_up(width + 2 * n_exp, LANES)
    total = n_exp * lax.axis_size("dp") * batches
    receives = sum(size(n_z, batches) for size in RECV.values())
    sends = 64 * n_z
    bf16 = jnp.bfloat16
    in_vmem = pl.BlockSpec(memory_space=pltpu.VMEM)
    anywhere = pl.BlockSpec(memory_space=pl.ANY)
    return pl.pallas_call(
        functools.partial(fused_kernel, n_exp),
        in_specs=[anywhere] * 6,
        out_specs=in_vmem,
        out_shape=pltpu.VMEM((n_rows, width), bf16),
        scratch_shapes=[
            pltpu.VMEM(expert_ids.shape[::-1], jnp.int32),
            pltpu.VMEM(gate_logits.shape[::-1], jnp.float32),
            pltpu.VMEM((n_rows, width), bf16),
            pltpu.VMEM((total, rows, lanes), bf16),
            pltpu.VMEM((total, rows, width), bf16),
            pltpu.VMEM((total // 2, rows, width), bf16),
            pltpu.VMEM((batches * n_z, rows, width), bf16),
            pltpu.VMEM((batches * n_z, rows, width), bf16),
            pltpu.VMEM((batches * n_z, rows // 2, width), bf16),
            pltpu.VMEM((batches * n_z, rows // 2, width), bf16),
            pltpu.VMEM((batches * (n_z + 1), rows, width), bf16),
            pltpu.VMEM((batches * (n_z + 1), rows, width), bf16),
            pltpu.VMEM((width, hidden_width), bf16),
            pltpu.VMEM((width, hidden_width), bf16),
            pltpu.VMEM((width, hidden_width), bf16),
            pltpu.SemaphoreType.DMA((sends,)),
            pltpu.SemaphoreType.DMA((receives,)),
            pltpu.SemaphoreType.DMA((6,)),
        ],
        compiler_params=pltpu.CompilerParams(
            collective_id=0, has_side_effects=True, vmem_limit_bytes=60 * 1024 * 1024
        ),
    )(tokens, expert_ids.T, gate_logits.T, w_gate[0], w_up[0], w_down[0].T)


def solution(mesh):
    def per_device(tokens, expert_ids, *others):
        n_exp = lax.axis_size("expert")
        if n_exp > 4 * expert_ids.shape[1]:
            return sparse_device(tokens, expert_ids, *others)
        paired = lax.axis_size("dp") == 4 and n_exp % 2 == 0 and tokens.shape[0] % 32 == 0
        return (fused_device if paired else dense_device)(tokens, expert_ids, *others)

    return jax.shard_map(
        per_device,
        mesh=mesh,
        in_specs=(
            P(("expert", "dp"), None),
            P(("expert", "dp"), None),
            P(("expert", "dp"), None),
            P("expert", None, "dp"),
            P("expert", None, "dp"),
            P("expert", "dp", None),
        ),
        out_specs=P(("expert", "dp"), None),
        check_vma=False,
    )
```

```python
import functools

import jax
import jax.numpy as jnp
from jax import lax
from jax.experimental import pallas as pl
from jax.experimental.pallas import tpu as pltpu
from jax.sharding import PartitionSpec as P


def expert_rows(tile_in, gate_w, up_w, down_w):
    gate_val = jnp.dot(tile_in, gate_w, preferred_element_type=jnp.float32)
    up_val = jnp.dot(tile_in, up_w, preferred_element_type=jnp.float32)
    hidden = ((up_val + 1.0) * gate_val * jax.nn.sigmoid(1.702 * gate_val)).astype(jnp.bfloat16)
    return jnp.dot(hidden, down_w, preferred_element_type=jnp.float32).astype(jnp.bfloat16)


def run_tiles(packed, first_row, last_row, gate_w, up_w, down_w):
    tile_rows = 128
    n_tiles = jnp.maximum(last_row - first_row + tile_rows - 1, 0) // tile_rows
    result_buf = jnp.zeros((packed.shape[0], down_w.shape[1]), jnp.bfloat16)

    def advance(index_t, buffer):
        at_row = first_row + index_t * tile_rows
        tile_in = lax.dynamic_slice_in_dim(packed, at_row, tile_rows, 0)
        return lax.dynamic_update_slice_in_dim(
            buffer, expert_rows(tile_in, gate_w, up_w, down_w), at_row, 0
        )

    return lax.fori_loop(0, n_tiles, advance, result_buf)


def sparse_device(tokens, expert_ids, gate_logits, w_gate, w_up, w_down):
    n_rows, width = tokens.shape
    n_tops = expert_ids.shape[1]
    n_exp = lax.axis_size("expert")
    n_dp = lax.axis_size("dp")
    slot_cap = max(2, 3 * n_rows * n_tops // (2 * n_exp))
    tile_rows = 128
    flat_ids = expert_ids.reshape(-1)
    onehot = (flat_ids[:, None] == jnp.arange(n_exp, dtype=jnp.int32)[None, :]).astype(jnp.int32)
    rank_in = jnp.sum((jnp.cumsum(onehot, axis=0) - onehot) * onehot, axis=1)
    counts = jnp.sum(onehot, axis=0)
    slot_idx = flat_ids * slot_cap + rank_in
    source = (
        jnp.zeros((n_exp * slot_cap,), jnp.int32)
        .at[slot_idx]
        .set(jnp.arange(n_rows * n_tops, dtype=jnp.int32) // n_tops)
    )
    filled = (jnp.arange(slot_cap)[None, :] < counts[:, None]).reshape(-1)
    outgoing = jnp.where(filled[:, None], tokens[source], jnp.zeros_like(tokens[source])).reshape(
        n_exp, slot_cap, width
    )
    rows_mid, counts_mid = (
        lax.all_to_all(outgoing, "expert", split_axis=0, concat_axis=0, tiled=True),
        lax.all_to_all(counts[:, None], "expert", split_axis=0, concat_axis=0, tiled=True),
    )
    rows_in, counts_in = (
        lax.all_gather(rows_mid, "dp", axis=0, tiled=True),
        lax.all_gather(counts_mid, "dp", axis=0, tiled=True),
    )
    rows_flat = rows_in.reshape(-1, width)
    total_rows = rows_flat.shape[0]
    live_row = (jnp.arange(slot_cap)[None, :] < counts_in.reshape(-1)[:, None]).reshape(-1)
    position = jnp.cumsum(live_row.astype(jnp.int32)) - 1
    live_total = jnp.sum(live_row.astype(jnp.int32))
    padded = (total_rows + tile_rows - 1) // tile_rows * tile_rows + tile_rows
    gather_idx = (
        jnp.zeros((padded,), jnp.int32)
        .at[jnp.where(live_row, position, padded)]
        .set(jnp.arange(total_rows, dtype=jnp.int32), mode="drop")
    )
    packed = rows_flat[gather_idx]
    gate_w = w_gate[0]
    up_w = w_up[0]
    down_w = w_down[0]
    merged = run_tiles(packed, 0, live_total, gate_w, up_w, down_w)
    slot_out = jnp.where(
        live_row[:, None],
        merged[jnp.where(live_row, position, 0)],
        jnp.zeros((total_rows, width), jnp.bfloat16),
    )
    summed = lax.psum_scatter(
        slot_out.reshape(n_dp * n_exp, slot_cap, width), "dp", scatter_dimension=0, tiled=True
    ).astype(jnp.float32)
    expert_out = lax.all_to_all(
        summed.astype(jnp.bfloat16), "expert", split_axis=0, concat_axis=0, tiled=True
    )
    picked = expert_out.reshape(n_exp * slot_cap, width)[slot_idx]
    gate_wts = jnp.exp(gate_logits)
    gate_wts = gate_wts / jnp.sum(gate_wts, axis=1, keepdims=True)
    mixed = jnp.sum(
        picked.reshape(n_rows, n_tops, width).astype(jnp.float32) * gate_wts[:, :, None], axis=1
    )
    return mixed.astype(jnp.bfloat16)


LANES = 128
CHUNKS = 1


def round_up(value, step):
    return (value + step - 1) // step * step


def routing_columns(expert_ids, gate_logits, n_exp, lanes):
    gate_wts = jnp.exp(gate_logits)
    gate_wts = gate_wts / jnp.sum(gate_wts, axis=1, keepdims=True)
    chosen = expert_ids[:, :, None] == jnp.arange(n_exp, dtype=jnp.int32)[None, None, :]
    by_expert = jnp.sum(jnp.where(chosen, gate_wts[:, :, None], 0.0), axis=1)
    high = by_expert.astype(jnp.bfloat16)
    low = (by_expert - high.astype(jnp.float32)).astype(jnp.bfloat16)
    columns = jnp.concatenate([high, low], axis=1)
    return jnp.pad(columns, ((0, 0), (0, lanes - columns.shape[1])))


def dense_kernel(n_exp, rows_ref, gate_ref, up_ref, down_ref, out_ref):
    width, hidden_width = gate_ref.shape
    lanes = rows_ref.shape[1]
    mine = lax.axis_index("expert")
    rows_in = rows_ref[:, :width]
    gate_val = jnp.dot(rows_in, gate_ref[...], preferred_element_type=jnp.float32)
    up_val = jnp.dot(rows_in, up_ref[...], preferred_element_type=jnp.float32)
    first = width // LANES * LANES
    extra = rows_ref[:, first:lanes].astype(jnp.float32)
    lane = lax.broadcasted_iota(jnp.int32, extra.shape, 1) + first - width
    weight = jnp.sum(jnp.where((lane == mine) | (lane == mine + n_exp), extra, 0.0), axis=1, keepdims=True)
    hidden = (up_val + 1.0) * gate_val * (weight / (1.0 + jnp.exp(-1.702 * gate_val)))
    out_ref[...] = jnp.dot(
        hidden.astype(jnp.bfloat16), down_ref[...], preferred_element_type=jnp.float32
    ).astype(out_ref.dtype)


def dense_rows(rows, gate_w, up_w, down_w, n_exp):
    n_rows, lanes = rows.shape
    width, hidden_width = gate_w.shape
    tile_rows = 256
    while n_rows % tile_rows:
        tile_rows //= 2
    whole = pl.BlockSpec(memory_space=pltpu.VMEM)
    return pl.pallas_call(
        functools.partial(dense_kernel, n_exp),
        grid=(n_rows // tile_rows,),
        in_specs=[pl.BlockSpec((tile_rows, lanes), lambda i: (i, 0)), whole, whole, whole],
        out_specs=pl.BlockSpec((tile_rows, width), lambda i: (i, 0)),
        out_shape=jax.ShapeDtypeStruct((n_rows, width), jnp.bfloat16),
        cost_estimate=pl.CostEstimate(
            flops=6 * n_rows * width * hidden_width,
            bytes_accessed=2 * n_rows * (lanes + width) + 6 * width * hidden_width,
            transcendentals=n_rows * hidden_width,
        ),
    )(rows, gate_w, up_w, down_w)


def dense_device(tokens, expert_ids, gate_logits, w_gate, w_up, w_down):
    n_rows, width = tokens.shape
    n_exp = lax.axis_size("expert")
    both = ("expert", "dp")
    lanes = round_up(width + 2 * n_exp, LANES)
    extra = routing_columns(expert_ids, gate_logits, n_exp, lanes - width)
    wide = jnp.concatenate([tokens, extra], axis=1)
    step = n_rows // CHUNKS
    done = []
    for chunk in range(CHUNKS):
        rows = lax.all_gather(wide[chunk * step : (chunk + 1) * step], both, axis=0, tiled=True)
        partial = dense_rows(rows, w_gate[0], w_up[0], w_down[0], n_exp)
        done.append(lax.psum_scatter(partial, both, scatter_dimension=0, tiled=True))
    return done[0] if CHUNKS == 1 else jnp.concatenate(done, axis=0)


def tile_product(n_exp, rows_in, extra, gate_ref, up_ref, down_ref):
    width = gate_ref.shape[0]
    mine = lax.axis_index("expert")
    gate_val = jnp.dot(rows_in, gate_ref[...], preferred_element_type=jnp.float32)
    up_val = jnp.dot(rows_in, up_ref[...], preferred_element_type=jnp.float32)
    extra = extra.astype(jnp.float32)
    lane = lax.broadcasted_iota(jnp.int32, extra.shape, 1) - width % LANES
    weight = jnp.sum(jnp.where((lane == mine) | (lane == mine + n_exp), extra, 0.0), axis=1, keepdims=True)
    hidden = (up_val + 1.0) * gate_val * (weight / (1.0 + jnp.exp(-1.702 * gate_val)))
    return lax.dot_general(
        hidden.astype(jnp.bfloat16),
        down_ref[...],
        (((1,), (1,)), ((), ())),
        preferred_element_type=jnp.float32,
    )


def fused_kernel(
    n_exp, tok_hbm, ids_hbm, logits_hbm, gate_hbm, up_hbm, down_hbm, out_ref,
    ids_ref, logits_ref, tok, held, part, core_in, sides_in, x_diag, y_diag, d_chain, o_chain,
    gate_ref, up_ref, down_ref, send_sem, recv_sem, load_sem,
):
    n_z = n_exp // 2
    reach = n_z // 2
    n_rows, width = out_ref.shape
    lanes = held.shape[2]
    rows = held.shape[1]
    batches = n_rows // rows
    half = rows // 2
    spare = width // LANES * LANES
    expert, dp = lax.axis_index("expert"), lax.axis_index("dp")
    z, y = lax.div(expert, 2), lax.rem(expert, 2)
    x, core = lax.div(dp, 2), lax.rem(dp, 2)
    to_x = (expert, (1 - x) * 2 + core)
    to_y = (z * 2 + 1 - y, dp)
    to_core = (expert, x * 2 + 1 - core)
    columns = {"o": y * 2 + x, "x": y * 2 + 1 - x, "y": (1 - y) * 2 + x, "d": (1 - y) * 2 + 1 - x}
    order = "oxyd"

    def to_z(place):
        return (place * 2 + y, dp)

    short = jnp.minimum(z, n_z - 1 - z)
    inward = jnp.where(z * 2 < n_z - 1, 1, -1)

    def near(i):
        if i == 0:
            return z
        paired = z - inward * ((i + 1) // 2) if i % 2 else z + inward * (i // 2)
        return jnp.where(i <= 2 * short, paired, z + inward * (i - short))

    class Plane:
        def __init__(self, i):
            self.i, self.zz = i, near(i)
            self.dist = jnp.abs(self.zz - z)
            self.away = jnp.where(self.zz < z, 1, -1)
            self.out = z + self.away
            self.back = z - self.away
            self.has_out = (self.out >= 0) & (self.out < n_z)
            self.maybe_far = i > reach
            self.far = self.dist > reach
            self.out_d = self.has_out & (self.dist < reach)

    planes = [Plane(i) for i in range(n_z)]
    others = range(1, n_z)

    def block(column, which, zz, h):
        return ((h * 4 + columns[column]) * 2 + which) * n_z + zz

    kinds = {}
    n_recv = [0]

    def recv_index(kind, at):
        if kind not in kinds:
            size = RECV[kind](n_z, batches)
            kinds[kind] = n_recv[0]
            n_recv[0] += size
        return kinds[kind] + at

    for kind in RECV:
        recv_index(kind, 0)

    def at(kind, h, zz):
        return recv_index(kind, h * n_z + zz)

    def at_core(h, column):
        return recv_index("core", h * 4 + order.index(column))

    def at_far(kind, h, i):
        return recv_index(kind, h * (n_z - reach) + (i - reach if i else 0))

    def at_chain(kind, h, slot):
        return recv_index(kind, h * (n_z + 1) + slot)

    sent = []

    def when(condition, action):
        if condition is None:
            action()
        else:
            pl.when(condition)(action)

    def start(index, source, target, device, condition=None):
        if len(sent) >= SENDS:
            before, oldest = sent[-SENDS]
            when(before, oldest.wait_send)
        copy = pltpu.make_async_remote_copy(
            src_ref=source,
            dst_ref=target,
            send_sem=send_sem.at[len(sent) % SENDS],
            recv_sem=recv_sem.at[index],
            device_id=device,
            device_id_type=pl.DeviceIdType.MESH,
        )
        sent.append((condition, copy))
        when(condition, copy.start)

    def arrived(index, target, condition=None):
        copy = pltpu.make_async_remote_copy(
            src_ref=target,
            dst_ref=target,
            send_sem=send_sem.at[0],
            recv_sem=recv_sem.at[index],
            device_id=to_core,
            device_id_type=pl.DeviceIdType.MESH,
        )
        when(condition, copy.wait_recv)

    above, below = z < n_z - 1, z > 0
    barrier = pltpu.get_barrier_semaphore()

    def greet(device):
        pl.semaphore_signal(barrier, inc=1, device_id=device, device_id_type=pl.DeviceIdType.MESH)

    for device in (to_x, to_y, to_core):
        greet(device)
    pl.when(above)(lambda: greet(to_z(z + 1)))
    pl.when(below)(lambda: greet(to_z(z - 1)))

    small = [
        pltpu.make_async_copy(source, target, load_sem.at[i])
        for i, (source, target) in enumerate(((ids_hbm, ids_ref), (logits_hbm, logits_ref), (tok_hbm, tok)))
    ]
    for load in small:
        load.start()
    loads = [
        pltpu.make_async_copy(source, target, load_sem.at[3 + i])
        for i, (source, target) in enumerate(((gate_hbm, gate_ref), (up_hbm, up_ref), (down_hbm, down_ref)))
    ]
    small[0].wait()
    small[1].wait()
    wts = jnp.exp(logits_ref[...])
    wts = wts / jnp.sum(wts, axis=0, keepdims=True)
    ids = ids_ref[...]
    by_expert = jnp.concatenate(
        [jnp.sum(jnp.where(ids == e, wts, 0.0), axis=0, keepdims=True) for e in range(n_exp)], axis=0
    )
    high = by_expert.astype(jnp.bfloat16).astype(jnp.float32)
    pairs = jnp.concatenate([high, by_expert - high], axis=0)
    filled = jnp.concatenate(
        [pairs, jnp.zeros((lanes - width - pairs.shape[0], n_rows), jnp.float32)], axis=0
    ).astype(jnp.bfloat16)
    eye = (
        lax.broadcasted_iota(jnp.int32, (n_rows, n_rows), 0)
        == lax.broadcasted_iota(jnp.int32, (n_rows, n_rows), 1)
    ).astype(jnp.float32).astype(jnp.bfloat16)
    extra_cols = lax.dot_general(
        eye, filled, (((1,), (1,)), ((), ())), preferred_element_type=jnp.float32
    ).astype(jnp.bfloat16)
    small[2].wait()
    for load in loads:
        load.start()
    for h in range(batches):
        own = block("o", core, z, h)
        held[own, :, :width] = tok[h * rows : (h + 1) * rows]
        held[own, :, width:] = extra_cols[h * rows : (h + 1) * rows]
    pl.semaphore_wait(barrier, 3 + above.astype(jnp.int32) + below.astype(jnp.int32))

    def send_own(h):
        own = held.at[block("o", core, z, h)]
        start(at("x", h, z), own, own, to_x)
        start(at("y", h, z), own, own, to_y)
        start(at("o", h, z), own, own, to_z(z + 1), above)
        start(at("o", h, z), own, own, to_z(z - 1), below)
        start(at_core(h, "o"), own, own, to_core)

    def take_x(h, i):
        p = planes[i]
        spot = block("x", core, p.zz, h)
        arrived(at("x", h, p.zz), held.at[spot])
        upper = held.at[spot, pl.ds(0, half)]
        if i == 0 or p.maybe_far:
            start(at_far("halves", h, i), upper, upper, to_y, p.far if i else None)
        start(at_core(h, "x"), held.at[spot], held.at[spot], to_core)

    def take_y(h, i):
        p = planes[i]
        spot = block("y", core, p.zz, h)
        arrived(at("y", h, p.zz), held.at[spot])
        lower = held.at[spot, pl.ds(half, half)]
        if i == 0 or p.maybe_far:
            start(at_far("halves", h, i), lower, lower, to_x, p.far if i else None)
        start(at_core(h, "y"), held.at[spot], held.at[spot], to_core)

    def take_xy(h, i):
        take_x(h, i)
        take_y(h, i)

    def take_o(h, i):
        p = planes[i]
        spot = held.at[block("o", core, p.zz, h)]
        arrived(at("o", h, p.zz), spot)
        start(at("o", h, p.zz), spot, spot, to_z(p.out), p.has_out)
        start(at("x", h, p.zz), spot, spot, to_x)
        start(at("y", h, p.zz), spot, spot, to_y)
        start(at_core(h, "o"), spot, spot, to_core)

    def take_d(h, i):
        p = planes[i]
        index = block("d", core, p.zz, h)
        spot = held.at[index]

        if i == 0:
            arrived(at_far("halves", h, i), spot)
            start(at("d", h, z), spot, spot, to_z(z + 1), above)
            start(at("d", h, z), spot, spot, to_z(z - 1), below)
        else:
            if p.maybe_far:
                arrived(at_far("halves", h, i), spot, p.far)
            arrived(at("d", h, p.zz), spot, p.dist <= reach if p.maybe_far else None)
            start(at("d", h, p.zz), spot, spot, to_z(p.out), p.out_d)
        start(at_core(h, "d"), spot, spot, to_core)

    loaded = []

    def product(h, column):
        arrived(at_core(h, column), held.at[pl.ds(block(column, 1 - core, 0, h), n_z)])
        if not loaded:
            for load in loads:
                load.wait()
            loaded.append(True)
        span = pl.ds(block(column, 0, 0, h), 2 * n_z)
        rows_in = held[span, :, :width].reshape(2 * n_z * rows, width)
        extra = held[span, :, spare:lanes].reshape(2 * n_z * rows, lanes - spare)
        result = tile_product(n_exp, rows_in, extra, gate_ref, up_ref, down_ref)
        part[span] = result.astype(part.dtype).reshape(2 * n_z, rows, width)
        start(
            recv_index("p", h * 4 + order.index(column)),
            part.at[pl.ds(block(column, 1 - core, 0, h), n_z)],
            core_in.at[pl.ds((h * 4 + order.index(column)) * n_z, n_z)],
            to_core,
        )

    def chained(chain, slot):
        chain[slot] = jnp.zeros(chain.shape[1:], chain.dtype)

    def clear():
        for h in range(batches):
            base = h * (n_z + 1)
            for p in planes[1:]:
                missing = (p.back < 0) | (p.back >= n_z)
                flipped = z + p.away
                no_up = (flipped < 0) | (flipped >= n_z)
                pl.when(no_up)(lambda p=p, base=base: chained(o_chain, base + p.zz))
                pl.when(no_up | (p.dist >= reach))(lambda p=p, base=base: chained(d_chain, base + p.zz))
                if p.maybe_far:

                    @pl.when(jnp.logical_not(p.far))
                    def _(p=p, h=h):
                        chained(x_diag, h * n_z + p.zz)
                        chained(y_diag, h * n_z + p.zz)

            for chain in (o_chain, d_chain):
                pl.when(z == 0)(lambda chain=chain, base=base: chained(chain, base + z))
                pl.when(z == n_z - 1)(lambda chain=chain, base=base: chained(chain, base + n_z))

    step = 16 if rows % 16 == 0 else rows

    def combined(h, column, zz, *more, target=None):
        spot = block(column, core, zz, h)
        place = (h * 4 + order.index(column)) * n_z + zz

        @pl.loop(0, rows // step)
        def _(k):
            span = pl.ds(k * step, step)
            total = part[spot, span].astype(jnp.float32) + core_in[place, span].astype(jnp.float32)
            for source, index in more:
                total = total + source[index, span].astype(jnp.float32)
            if target is None:
                part[spot, span] = total.astype(part.dtype)
            else:
                out_ref[pl.ds(target + k * step, step)] = total.astype(out_ref.dtype)

        return spot

    seen = set()

    def need(h, column):
        if (h, column) not in seen:
            seen.add((h, column))
            base = (h * 4 + order.index(column)) * n_z
            arrived(recv_index("p", h * 4 + order.index(column)), core_in.at[pl.ds(base, n_z)])

    def slot_at(p):
        toward = z - p.away
        return jnp.where((toward == p.zz) & (p.away > 0), n_z, p.zz)

    def give_d(h, i):
        p = planes[i]
        base = h * (n_z + 1)
        need(h, "d")
        if i == 0:
            arrived(at_chain("dc", h, z), d_chain.at[base + z], below)
            arrived(at_chain("dc", h, n_z), d_chain.at[base + n_z], above)
            spot = combined(h, "d", z, (d_chain, base + z), (d_chain, base + n_z))
        else:
            has_up = p.has_out & (p.dist < reach)
            arrived(at_chain("dc", h, p.zz), d_chain.at[base + p.zz], has_up)
            spot = combined(h, "d", p.zz, (d_chain, base + p.zz))
            start(
                at_chain("dc", h, slot_at(p)), part.at[spot], d_chain.at[base + slot_at(p)], to_z(p.back),
                jnp.logical_not(p.far) if p.maybe_far else None,
            )
        if i == 0 or p.maybe_far:
            condition = p.far if i else None
            start(at_far("dx", h, i), part.at[spot, pl.ds(half, half)], x_diag.at[h * n_z + p.zz], to_x, condition)
            start(at_far("dy", h, i), part.at[spot, pl.ds(0, half)], y_diag.at[h * n_z + p.zz], to_y, condition)

    def give_x(h, i):
        p = planes[i]
        need(h, "x")
        index = h * n_z + p.zz
        spot = combined(h, "x", p.zz)
        if i == 0 or p.maybe_far:
            arrived(at_far("dy", h, i), y_diag.at[index], p.far if i else None)
            part[spot, :half] = (
                part[spot, :half].astype(jnp.float32) + y_diag[index].astype(jnp.float32)
            ).astype(part.dtype)
        start(at("sides", h, p.zz), part.at[spot], sides_in.at[2 * index], to_x)

    def give_y(h, i):
        p = planes[i]
        need(h, "y")
        index = h * n_z + p.zz
        spot = combined(h, "y", p.zz)
        if i == 0 or p.maybe_far:
            arrived(at_far("dx", h, i), x_diag.at[index], p.far if i else None)
            part[spot, half:] = (
                part[spot, half:].astype(jnp.float32) + x_diag[index].astype(jnp.float32)
            ).astype(part.dtype)
        start(at("sides", h, p.zz), part.at[spot], sides_in.at[2 * index + 1], to_y)

    def give_xy(h, i):
        give_x(h, i)
        give_y(h, i)

    def give_o(h, i):
        p = planes[i]
        base = h * (n_z + 1)
        index = h * n_z + p.zz
        need(h, "o")
        arrived(at("sides", h, p.zz), sides_in.at[pl.ds(2 * index, 2)])
        if i == 0:
            arrived(at_chain("oc", h, z), o_chain.at[base + z], below)
            arrived(at_chain("oc", h, n_z), o_chain.at[base + n_z], above)
            combined(
                h, "o", z, (sides_in, 2 * index), (sides_in, 2 * index + 1), (o_chain, base + z), (o_chain, base + n_z),
                target=h * rows,
            )
        else:
            arrived(at_chain("oc", h, p.zz), o_chain.at[base + p.zz], p.has_out)
            spot = combined(h, "o", p.zz, (sides_in, 2 * index), (sides_in, 2 * index + 1), (o_chain, base + p.zz))
            start(at_chain("oc", h, slot_at(p)), part.at[spot], o_chain.at[base + slot_at(p)], to_z(p.back))

    steps = {
        "own": send_own, "clear": clear, "x": take_x, "y": take_y, "xy": take_xy, "o": take_o, "d": take_d,
        "C": product, "Rd": give_d, "Rx": give_x, "Ry": give_y, "Rxy": give_xy, "Ro": give_o,
    }
    for name, *numbers in PLAN:
        steps[name](*numbers)
    for condition, copy in sent[-SENDS:]:
        when(condition, copy.wait_send)


RECV = {kind: (lambda n_z, batches: n_z * batches) for kind in ("x", "y", "o", "d", "sides")}
RECV["halves"] = RECV["dx"] = RECV["dy"] = lambda n_z, batches: (n_z - n_z // 2) * batches
RECV["core"] = RECV["p"] = lambda n_z, batches: 4 * batches
RECV["dc"] = RECV["oc"] = lambda n_z, batches: (n_z + 1) * batches
SENDS = 48

BATCHES = 2

PLAN = (
    ("own", 0),
    ("clear",),
    ("own", 1),
    ("x", 0, 0),
    ("y", 0, 0),
    ("o", 0, 1),
    ("o", 0, 2),
    ("x", 1, 0),
    ("y", 1, 0),
    ("d", 0, 0),
    ("o", 0, 3),
    ("y", 0, 1),
    ("o", 1, 1),
    ("x", 0, 1),
    ("C", 0, "o"),
    ("y", 0, 2),
    ("d", 0, 1),
    ("d", 0, 2),
    ("x", 0, 2),
    ("y", 0, 3),
    ("x", 0, 3),
    ("o", 1, 3),
    ("d", 0, 3),
    ("C", 0, "y"),
    ("o", 1, 2),
    ("d", 1, 0),
    ("y", 1, 1),
    ("C", 0, "d"),
    ("y", 1, 3),
    ("x", 1, 3),
    ("C", 0, "x"),
    ("Rd", 0, 3),
    ("Ry", 0, 2),
    ("Ry", 0, 1),
    ("d", 1, 2),
    ("d", 1, 1),
    ("Rd", 0, 2),
    ("d", 1, 3),
    ("Rx", 0, 1),
    ("Rd", 0, 1),
    ("x", 1, 2),
    ("y", 1, 2),
    ("Rx", 0, 2),
    ("x", 1, 1),
    ("C", 1, "d"),
    ("Rx", 0, 3),
    ("C", 1, "x"),
    ("Rd", 1, 3),
    ("Rd", 1, 2),
    ("Ry", 0, 3),
    ("C", 1, "y"),
    ("Ro", 0, 2),
    ("Rd", 0, 0),
    ("Rx", 1, 3),
    ("Rx", 1, 2),
    ("Rx", 1, 1),
    ("Rd", 1, 1),
    ("Ry", 1, 3),
    ("Ry", 1, 2),
    ("Ry", 1, 1),
    ("C", 1, "o"),
    ("Ro", 0, 3),
    ("Ro", 1, 3),
    ("Rd", 1, 0),
    ("Rx", 0, 0),
    ("Ry", 0, 0),
    ("Ro", 1, 2),
    ("Ro", 0, 1),
    ("Ro", 1, 1),
    ("Rx", 1, 0),
    ("Ry", 1, 0),
    ("Ro", 0, 0),
    ("Ro", 1, 0),
)


def fused_device(tokens, expert_ids, gate_logits, w_gate, w_up, w_down):
    n_rows, width = tokens.shape
    hidden_width = w_gate.shape[2]
    n_exp = lax.axis_size("expert")
    n_z = n_exp // 2
    batches = BATCHES
    rows = n_rows // batches
    lanes = round_up(width + 2 * n_exp, LANES)
    total = n_exp * lax.axis_size("dp") * batches
    receives = sum(size(n_z, batches) for size in RECV.values())
    bf16 = jnp.bfloat16
    in_vmem = pl.BlockSpec(memory_space=pltpu.VMEM)
    anywhere = pl.BlockSpec(memory_space=pl.ANY)
    return pl.pallas_call(
        functools.partial(fused_kernel, n_exp),
        in_specs=[anywhere] * 6,
        out_specs=in_vmem,
        out_shape=pltpu.VMEM((n_rows, width), bf16),
        scratch_shapes=[
            pltpu.VMEM(expert_ids.shape[::-1], jnp.int32),
            pltpu.VMEM(gate_logits.shape[::-1], jnp.float32),
            pltpu.VMEM((n_rows, width), bf16),
            pltpu.VMEM((total, rows, lanes), bf16),
            pltpu.VMEM((total, rows, width), bf16),
            pltpu.VMEM((total // 2, rows, width), bf16),
            pltpu.VMEM((batches * n_z * 2, rows, width), bf16),
            pltpu.VMEM((batches * n_z, rows // 2, width), bf16),
            pltpu.VMEM((batches * n_z, rows // 2, width), bf16),
            pltpu.VMEM((batches * (n_z + 1), rows, width), bf16),
            pltpu.VMEM((batches * (n_z + 1), rows, width), bf16),
            pltpu.VMEM((width, hidden_width), bf16),
            pltpu.VMEM((width, hidden_width), bf16),
            pltpu.VMEM((width, hidden_width), bf16),
            pltpu.SemaphoreType.DMA((SENDS,)),
            pltpu.SemaphoreType.DMA((receives,)),
            pltpu.SemaphoreType.DMA((6,)),
        ],
        compiler_params=pltpu.CompilerParams(
            collective_id=0, has_side_effects=True, vmem_limit_bytes=60 * 1024 * 1024
        ),
    )(tokens, expert_ids.T, gate_logits.T, w_gate[0], w_up[0], w_down[0].T)


def solution(mesh):
    def per_device(tokens, expert_ids, *others):
        n_exp = lax.axis_size("expert")
        if n_exp > 4 * expert_ids.shape[1]:
            return sparse_device(tokens, expert_ids, *others)
        paired = lax.axis_size("dp") == 4 and n_exp % 2 == 0 and tokens.shape[0] % 32 == 0
        return (fused_device if paired else dense_device)(tokens, expert_ids, *others)

    return jax.shard_map(
        per_device,
        mesh=mesh,
        in_specs=(
            P(("expert", "dp"), None),
            P(("expert", "dp"), None),
            P(("expert", "dp"), None),
            P("expert", None, "dp"),
            P("expert", None, "dp"),
            P("expert", "dp", None),
        ),
        out_specs=P(("expert", "dp"), None),
        check_vma=False,
    )
```

```python
import functools

import jax
import jax.numpy as jnp
from jax import lax
from jax.experimental import pallas as pl
from jax.experimental.pallas import tpu as pltpu
from jax.sharding import PartitionSpec as P


def expert_rows(tile_in, gate_w, up_w, down_w):
    gate_val = jnp.dot(tile_in, gate_w, preferred_element_type=jnp.float32)
    up_val = jnp.dot(tile_in, up_w, preferred_element_type=jnp.float32)
    hidden = ((up_val + 1.0) * gate_val * jax.nn.sigmoid(1.702 * gate_val)).astype(jnp.bfloat16)
    return jnp.dot(hidden, down_w, preferred_element_type=jnp.float32).astype(jnp.bfloat16)


def run_tiles(packed, first_row, last_row, gate_w, up_w, down_w):
    tile_rows = 128
    n_tiles = jnp.maximum(last_row - first_row + tile_rows - 1, 0) // tile_rows
    result_buf = jnp.zeros((packed.shape[0], down_w.shape[1]), jnp.bfloat16)

    def advance(index_t, buffer):
        at_row = first_row + index_t * tile_rows
        tile_in = lax.dynamic_slice_in_dim(packed, at_row, tile_rows, 0)
        return lax.dynamic_update_slice_in_dim(
            buffer, expert_rows(tile_in, gate_w, up_w, down_w), at_row, 0
        )

    return lax.fori_loop(0, n_tiles, advance, result_buf)


def sparse_device(tokens, expert_ids, gate_logits, w_gate, w_up, w_down):
    n_rows, width = tokens.shape
    n_tops = expert_ids.shape[1]
    n_exp = lax.axis_size("expert")
    n_dp = lax.axis_size("dp")
    slot_cap = max(2, 3 * n_rows * n_tops // (2 * n_exp))
    tile_rows = 128
    flat_ids = expert_ids.reshape(-1)
    onehot = (flat_ids[:, None] == jnp.arange(n_exp, dtype=jnp.int32)[None, :]).astype(jnp.int32)
    rank_in = jnp.sum((jnp.cumsum(onehot, axis=0) - onehot) * onehot, axis=1)
    counts = jnp.sum(onehot, axis=0)
    slot_idx = flat_ids * slot_cap + rank_in
    source = (
        jnp.zeros((n_exp * slot_cap,), jnp.int32)
        .at[slot_idx]
        .set(jnp.arange(n_rows * n_tops, dtype=jnp.int32) // n_tops)
    )
    filled = (jnp.arange(slot_cap)[None, :] < counts[:, None]).reshape(-1)
    outgoing = jnp.where(filled[:, None], tokens[source], jnp.zeros_like(tokens[source])).reshape(
        n_exp, slot_cap, width
    )
    rows_mid, counts_mid = (
        lax.all_to_all(outgoing, "expert", split_axis=0, concat_axis=0, tiled=True),
        lax.all_to_all(counts[:, None], "expert", split_axis=0, concat_axis=0, tiled=True),
    )
    rows_in, counts_in = (
        lax.all_gather(rows_mid, "dp", axis=0, tiled=True),
        lax.all_gather(counts_mid, "dp", axis=0, tiled=True),
    )
    rows_flat = rows_in.reshape(-1, width)
    total_rows = rows_flat.shape[0]
    live_row = (jnp.arange(slot_cap)[None, :] < counts_in.reshape(-1)[:, None]).reshape(-1)
    position = jnp.cumsum(live_row.astype(jnp.int32)) - 1
    live_total = jnp.sum(live_row.astype(jnp.int32))
    padded = (total_rows + tile_rows - 1) // tile_rows * tile_rows + tile_rows
    gather_idx = (
        jnp.zeros((padded,), jnp.int32)
        .at[jnp.where(live_row, position, padded)]
        .set(jnp.arange(total_rows, dtype=jnp.int32), mode="drop")
    )
    packed = rows_flat[gather_idx]
    gate_w = w_gate[0]
    up_w = w_up[0]
    down_w = w_down[0]
    merged = run_tiles(packed, 0, live_total, gate_w, up_w, down_w)
    slot_out = jnp.where(
        live_row[:, None],
        merged[jnp.where(live_row, position, 0)],
        jnp.zeros((total_rows, width), jnp.bfloat16),
    )
    summed = lax.psum_scatter(
        slot_out.reshape(n_dp * n_exp, slot_cap, width), "dp", scatter_dimension=0, tiled=True
    ).astype(jnp.float32)
    expert_out = lax.all_to_all(
        summed.astype(jnp.bfloat16), "expert", split_axis=0, concat_axis=0, tiled=True
    )
    picked = expert_out.reshape(n_exp * slot_cap, width)[slot_idx]
    gate_wts = jnp.exp(gate_logits)
    gate_wts = gate_wts / jnp.sum(gate_wts, axis=1, keepdims=True)
    mixed = jnp.sum(
        picked.reshape(n_rows, n_tops, width).astype(jnp.float32) * gate_wts[:, :, None], axis=1
    )
    return mixed.astype(jnp.bfloat16)


LANES = 128
CHUNKS = 1


def round_up(value, step):
    return (value + step - 1) // step * step


def routing_columns(expert_ids, gate_logits, n_exp, lanes):
    gate_wts = jnp.exp(gate_logits)
    gate_wts = gate_wts / jnp.sum(gate_wts, axis=1, keepdims=True)
    chosen = expert_ids[:, :, None] == jnp.arange(n_exp, dtype=jnp.int32)[None, None, :]
    by_expert = jnp.sum(jnp.where(chosen, gate_wts[:, :, None], 0.0), axis=1)
    high = by_expert.astype(jnp.bfloat16)
    low = (by_expert - high.astype(jnp.float32)).astype(jnp.bfloat16)
    columns = jnp.concatenate([high, low], axis=1)
    return jnp.pad(columns, ((0, 0), (0, lanes - columns.shape[1])))


def dense_kernel(n_exp, rows_ref, gate_ref, up_ref, down_ref, out_ref):
    width, hidden_width = gate_ref.shape
    lanes = rows_ref.shape[1]
    mine = lax.axis_index("expert")
    rows_in = rows_ref[:, :width]
    gate_val = jnp.dot(rows_in, gate_ref[...], preferred_element_type=jnp.float32)
    up_val = jnp.dot(rows_in, up_ref[...], preferred_element_type=jnp.float32)
    first = width // LANES * LANES
    extra = rows_ref[:, first:lanes].astype(jnp.float32)
    lane = lax.broadcasted_iota(jnp.int32, extra.shape, 1) + first - width
    weight = jnp.sum(jnp.where((lane == mine) | (lane == mine + n_exp), extra, 0.0), axis=1, keepdims=True)
    hidden = (up_val + 1.0) * gate_val * (weight / (1.0 + jnp.exp(-1.702 * gate_val)))
    out_ref[...] = jnp.dot(
        hidden.astype(jnp.bfloat16), down_ref[...], preferred_element_type=jnp.float32
    ).astype(out_ref.dtype)


def dense_rows(rows, gate_w, up_w, down_w, n_exp):
    n_rows, lanes = rows.shape
    width, hidden_width = gate_w.shape
    tile_rows = 256
    while n_rows % tile_rows:
        tile_rows //= 2
    whole = pl.BlockSpec(memory_space=pltpu.VMEM)
    return pl.pallas_call(
        functools.partial(dense_kernel, n_exp),
        grid=(n_rows // tile_rows,),
        in_specs=[pl.BlockSpec((tile_rows, lanes), lambda i: (i, 0)), whole, whole, whole],
        out_specs=pl.BlockSpec((tile_rows, width), lambda i: (i, 0)),
        out_shape=jax.ShapeDtypeStruct((n_rows, width), jnp.bfloat16),
        cost_estimate=pl.CostEstimate(
            flops=6 * n_rows * width * hidden_width,
            bytes_accessed=2 * n_rows * (lanes + width) + 6 * width * hidden_width,
            transcendentals=n_rows * hidden_width,
        ),
    )(rows, gate_w, up_w, down_w)


def dense_device(tokens, expert_ids, gate_logits, w_gate, w_up, w_down):
    n_rows, width = tokens.shape
    n_exp = lax.axis_size("expert")
    both = ("expert", "dp")
    lanes = round_up(width + 2 * n_exp, LANES)
    extra = routing_columns(expert_ids, gate_logits, n_exp, lanes - width)
    wide = jnp.concatenate([tokens, extra], axis=1)
    step = n_rows // CHUNKS
    done = []
    for chunk in range(CHUNKS):
        rows = lax.all_gather(wide[chunk * step : (chunk + 1) * step], both, axis=0, tiled=True)
        partial = dense_rows(rows, w_gate[0], w_up[0], w_down[0], n_exp)
        done.append(lax.psum_scatter(partial, both, scatter_dimension=0, tiled=True))
    return done[0] if CHUNKS == 1 else jnp.concatenate(done, axis=0)


def tile_product(n_exp, rows_in, extra, gate_ref, up_ref, down_ref):
    width = gate_ref.shape[0]
    mine = lax.axis_index("expert")
    gate_val = jnp.dot(rows_in, gate_ref[...], preferred_element_type=jnp.float32)
    up_val = jnp.dot(rows_in, up_ref[...], preferred_element_type=jnp.float32)
    extra = extra.astype(jnp.float32)
    lane = lax.broadcasted_iota(jnp.int32, extra.shape, 1) - width % LANES
    weight = jnp.sum(jnp.where((lane == mine) | (lane == mine + n_exp), extra, 0.0), axis=1, keepdims=True)
    hidden = (up_val + 1.0) * gate_val * (weight / (1.0 + jnp.exp(-1.702 * gate_val)))
    return lax.dot_general(
        hidden.astype(jnp.bfloat16),
        down_ref[...],
        (((1,), (1,)), ((), ())),
        preferred_element_type=jnp.float32,
    )


def fused_kernel(
    n_exp, tok_hbm, ids_hbm, logits_hbm, gate_hbm, up_hbm, down_hbm, out_ref,
    ids_ref, logits_ref, tok, held, part, core_in, sides_in, x_diag, y_diag, d_chain, o_chain,
    gate_ref, up_ref, down_ref, send_sem, recv_sem, load_sem,
):
    n_z = n_exp // 2
    reach = n_z // 2
    n_rows, width = out_ref.shape
    lanes = held.shape[2]
    rows = held.shape[1]
    batches = n_rows // rows
    half = rows // 2
    spare = width // LANES * LANES
    expert, dp = lax.axis_index("expert"), lax.axis_index("dp")
    z, y = lax.div(expert, 2), lax.rem(expert, 2)
    x, core = lax.div(dp, 2), lax.rem(dp, 2)
    to_x = (expert, (1 - x) * 2 + core)
    to_y = (z * 2 + 1 - y, dp)
    to_core = (expert, x * 2 + 1 - core)
    columns = {"o": y * 2 + x, "x": y * 2 + 1 - x, "y": (1 - y) * 2 + x, "d": (1 - y) * 2 + 1 - x}
    order = "oxyd"

    def to_z(place):
        return (place * 2 + y, dp)

    short = jnp.minimum(z, n_z - 1 - z)
    inward = jnp.where(z * 2 < n_z - 1, 1, -1)

    def near(i):
        if i == 0:
            return z
        paired = z - inward * ((i + 1) // 2) if i % 2 else z + inward * (i // 2)
        return jnp.where(i <= 2 * short, paired, z + inward * (i - short))

    class Plane:
        def __init__(self, i):
            self.i, self.zz = i, near(i)
            self.dist = jnp.abs(self.zz - z)
            self.away = jnp.where(self.zz < z, 1, -1)
            self.out = z + self.away
            self.back = z - self.away
            self.has_out = (self.out >= 0) & (self.out < n_z)
            self.maybe_far = i > reach
            self.far = self.dist > reach
            self.out_d = self.has_out & (self.dist < reach)

    planes = [Plane(i) for i in range(n_z)]
    others = range(1, n_z)

    def block(column, which, zz, h):
        return ((h * 4 + columns[column]) * 2 + which) * n_z + zz

    kinds = {}
    n_recv = [0]

    def recv_index(kind, at):
        if kind not in kinds:
            size = RECV[kind](n_z, batches)
            kinds[kind] = n_recv[0]
            n_recv[0] += size
        return kinds[kind] + at

    for kind in RECV:
        recv_index(kind, 0)

    def at(kind, h, zz):
        return recv_index(kind, h * n_z + zz)

    def at_core(h, column):
        return recv_index("core", h * 4 + order.index(column))

    def at_far(kind, h, i):
        return recv_index(kind, h * (n_z - reach) + (i - reach if i else 0))

    def at_chain(kind, h, slot):
        return recv_index(kind, h * (n_z + 1) + slot)

    sent = []

    def when(condition, action):
        if condition is None:
            action()
        else:
            pl.when(condition)(action)

    def start(index, source, target, device, condition=None):
        if len(sent) >= SENDS:
            before, oldest = sent[-SENDS]
            when(before, oldest.wait_send)
        copy = pltpu.make_async_remote_copy(
            src_ref=source,
            dst_ref=target,
            send_sem=send_sem.at[len(sent) % SENDS],
            recv_sem=recv_sem.at[index],
            device_id=device,
            device_id_type=pl.DeviceIdType.MESH,
        )
        sent.append((condition, copy))
        when(condition, copy.start)

    def arrived(index, target, condition=None):
        copy = pltpu.make_async_remote_copy(
            src_ref=target,
            dst_ref=target,
            send_sem=send_sem.at[0],
            recv_sem=recv_sem.at[index],
            device_id=to_core,
            device_id_type=pl.DeviceIdType.MESH,
        )
        when(condition, copy.wait_recv)

    above, below = z < n_z - 1, z > 0
    barrier = pltpu.get_barrier_semaphore()

    def greet(device):
        pl.semaphore_signal(barrier, inc=1, device_id=device, device_id_type=pl.DeviceIdType.MESH)

    for device in (to_x, to_y, to_core):
        greet(device)
    pl.when(above)(lambda: greet(to_z(z + 1)))
    pl.when(below)(lambda: greet(to_z(z - 1)))

    small = [
        pltpu.make_async_copy(source, target, load_sem.at[i])
        for i, (source, target) in enumerate(((ids_hbm, ids_ref), (logits_hbm, logits_ref), (tok_hbm, tok)))
    ]
    for load in small:
        load.start()
    loads = [
        pltpu.make_async_copy(source, target, load_sem.at[3 + i])
        for i, (source, target) in enumerate(((gate_hbm, gate_ref), (up_hbm, up_ref), (down_hbm, down_ref)))
    ]
    small[0].wait()
    small[1].wait()
    wts = jnp.exp(logits_ref[...])
    wts = wts / jnp.sum(wts, axis=0, keepdims=True)
    ids = ids_ref[...]
    by_expert = jnp.concatenate(
        [jnp.sum(jnp.where(ids == e, wts, 0.0), axis=0, keepdims=True) for e in range(n_exp)], axis=0
    )
    high = by_expert.astype(jnp.bfloat16).astype(jnp.float32)
    pairs = jnp.concatenate([high, by_expert - high], axis=0)
    filled = jnp.concatenate(
        [pairs, jnp.zeros((lanes - width - pairs.shape[0], n_rows), jnp.float32)], axis=0
    ).astype(jnp.bfloat16)
    eye = (
        lax.broadcasted_iota(jnp.int32, (n_rows, n_rows), 0)
        == lax.broadcasted_iota(jnp.int32, (n_rows, n_rows), 1)
    ).astype(jnp.float32).astype(jnp.bfloat16)
    extra_cols = lax.dot_general(
        eye, filled, (((1,), (1,)), ((), ())), preferred_element_type=jnp.float32
    ).astype(jnp.bfloat16)
    small[2].wait()
    for load in loads:
        load.start()
    for h in range(batches):
        own = block("o", core, z, h)
        held[own, :, :width] = tok[h * rows : (h + 1) * rows]
        held[own, :, width:] = extra_cols[h * rows : (h + 1) * rows]
    pl.semaphore_wait(barrier, 3 + above.astype(jnp.int32) + below.astype(jnp.int32))

    def send_own(h):
        own = held.at[block("o", core, z, h)]
        start(at("x", h, z), own, own, to_x)
        start(at("y", h, z), own, own, to_y)
        start(at("o", h, z), own, own, to_z(z + 1), above)
        start(at("o", h, z), own, own, to_z(z - 1), below)
        start(at_core(h, "o"), own, own, to_core)

    def take_x(h, i):
        p = planes[i]
        spot = block("x", core, p.zz, h)
        arrived(at("x", h, p.zz), held.at[spot])
        upper = held.at[spot, pl.ds(0, half)]
        if i == 0 or p.maybe_far:
            start(at_far("halves", h, i), upper, upper, to_y, p.far if i else None)
        start(at_core(h, "x"), held.at[spot], held.at[spot], to_core)

    def take_y(h, i):
        p = planes[i]
        spot = block("y", core, p.zz, h)
        arrived(at("y", h, p.zz), held.at[spot])
        lower = held.at[spot, pl.ds(half, half)]
        if i == 0 or p.maybe_far:
            start(at_far("halves", h, i), lower, lower, to_x, p.far if i else None)
        start(at_core(h, "y"), held.at[spot], held.at[spot], to_core)

    def take_xy(h, i):
        take_x(h, i)
        take_y(h, i)

    def take_o(h, i):
        p = planes[i]
        spot = held.at[block("o", core, p.zz, h)]
        arrived(at("o", h, p.zz), spot)
        start(at("o", h, p.zz), spot, spot, to_z(p.out), p.has_out)
        start(at("x", h, p.zz), spot, spot, to_x)
        start(at("y", h, p.zz), spot, spot, to_y)
        start(at_core(h, "o"), spot, spot, to_core)

    def take_d(h, i):
        p = planes[i]
        index = block("d", core, p.zz, h)
        spot = held.at[index]

        if i == 0:
            arrived(at_far("halves", h, i), spot)
            start(at("d", h, z), spot, spot, to_z(z + 1), above)
            start(at("d", h, z), spot, spot, to_z(z - 1), below)
        else:
            if p.maybe_far:
                arrived(at_far("halves", h, i), spot, p.far)
            arrived(at("d", h, p.zz), spot, p.dist <= reach if p.maybe_far else None)
            start(at("d", h, p.zz), spot, spot, to_z(p.out), p.out_d)
        start(at_core(h, "d"), spot, spot, to_core)

    loaded = []

    def product(h, column):
        arrived(at_core(h, column), held.at[pl.ds(block(column, 1 - core, 0, h), n_z)])
        if not loaded:
            for load in loads:
                load.wait()
            loaded.append(True)
        span = pl.ds(block(column, 0, 0, h), 2 * n_z)
        rows_in = held[span, :, :width].reshape(2 * n_z * rows, width)
        extra = held[span, :, spare:lanes].reshape(2 * n_z * rows, lanes - spare)
        result = tile_product(n_exp, rows_in, extra, gate_ref, up_ref, down_ref)
        part[span] = result.astype(part.dtype).reshape(2 * n_z, rows, width)
        start(
            recv_index("p", h * 4 + order.index(column)),
            part.at[pl.ds(block(column, 1 - core, 0, h), n_z)],
            core_in.at[pl.ds((h * 4 + order.index(column)) * n_z, n_z)],
            to_core,
        )

    def chained(chain, slot):
        chain[slot] = jnp.zeros(chain.shape[1:], chain.dtype)

    def clear():
        for h in range(batches):
            base = h * (n_z + 1)
            for p in planes[1:]:
                missing = (p.back < 0) | (p.back >= n_z)
                flipped = z + p.away
                no_up = (flipped < 0) | (flipped >= n_z)
                pl.when(no_up)(lambda p=p, base=base: chained(o_chain, base + p.zz))
                pl.when(no_up | (p.dist >= reach))(lambda p=p, base=base: chained(d_chain, base + p.zz))
                if p.maybe_far:

                    @pl.when(jnp.logical_not(p.far))
                    def _(p=p, h=h):
                        chained(x_diag, h * n_z + p.zz)
                        chained(y_diag, h * n_z + p.zz)

            for chain in (o_chain, d_chain):
                pl.when(z == 0)(lambda chain=chain, base=base: chained(chain, base + z))
                pl.when(z == n_z - 1)(lambda chain=chain, base=base: chained(chain, base + n_z))

    step = 16 if rows % 16 == 0 else rows

    def combined(h, column, zz, *more, target=None):
        spot = block(column, core, zz, h)
        place = (h * 4 + order.index(column)) * n_z + zz

        @pl.loop(0, rows // step)
        def _(k):
            span = pl.ds(k * step, step)
            total = part[spot, span].astype(jnp.float32) + core_in[place, span].astype(jnp.float32)
            for source, index in more:
                total = total + source[index, span].astype(jnp.float32)
            if target is None:
                part[spot, span] = total.astype(part.dtype)
            else:
                out_ref[pl.ds(target + k * step, step)] = total.astype(out_ref.dtype)

        return spot

    seen = set()

    def need(h, column):
        if (h, column) not in seen:
            seen.add((h, column))
            base = (h * 4 + order.index(column)) * n_z
            arrived(recv_index("p", h * 4 + order.index(column)), core_in.at[pl.ds(base, n_z)])

    def slot_at(p):
        toward = z - p.away
        return jnp.where((toward == p.zz) & (p.away > 0), n_z, p.zz)

    def give_d(h, i):
        p = planes[i]
        base = h * (n_z + 1)
        need(h, "d")
        if i == 0:
            arrived(at_chain("dc", h, z), d_chain.at[base + z], below)
            arrived(at_chain("dc", h, n_z), d_chain.at[base + n_z], above)
            spot = combined(h, "d", z, (d_chain, base + z), (d_chain, base + n_z))
        else:
            has_up = p.has_out & (p.dist < reach)
            arrived(at_chain("dc", h, p.zz), d_chain.at[base + p.zz], has_up)
            spot = combined(h, "d", p.zz, (d_chain, base + p.zz))
            start(
                at_chain("dc", h, slot_at(p)), part.at[spot], d_chain.at[base + slot_at(p)], to_z(p.back),
                jnp.logical_not(p.far) if p.maybe_far else None,
            )
        if i == 0 or p.maybe_far:
            condition = p.far if i else None
            start(at_far("dx", h, i), part.at[spot, pl.ds(half, half)], x_diag.at[h * n_z + p.zz], to_x, condition)
            start(at_far("dy", h, i), part.at[spot, pl.ds(0, half)], y_diag.at[h * n_z + p.zz], to_y, condition)

    def give_x(h, i):
        p = planes[i]
        need(h, "x")
        index = h * n_z + p.zz
        spot = combined(h, "x", p.zz)
        if i == 0 or p.maybe_far:
            arrived(at_far("dy", h, i), y_diag.at[index], p.far if i else None)
            part[spot, :half] = (
                part[spot, :half].astype(jnp.float32) + y_diag[index].astype(jnp.float32)
            ).astype(part.dtype)
        start(at("sides", h, p.zz), part.at[spot], sides_in.at[2 * index], to_x)

    def give_y(h, i):
        p = planes[i]
        need(h, "y")
        index = h * n_z + p.zz
        spot = combined(h, "y", p.zz)
        if i == 0 or p.maybe_far:
            arrived(at_far("dx", h, i), x_diag.at[index], p.far if i else None)
            part[spot, half:] = (
                part[spot, half:].astype(jnp.float32) + x_diag[index].astype(jnp.float32)
            ).astype(part.dtype)
        start(at("sides", h, p.zz), part.at[spot], sides_in.at[2 * index + 1], to_y)

    def give_xy(h, i):
        give_x(h, i)
        give_y(h, i)

    def give_o(h, i):
        p = planes[i]
        base = h * (n_z + 1)
        index = h * n_z + p.zz
        need(h, "o")
        arrived(at("sides", h, p.zz), sides_in.at[pl.ds(2 * index, 2)])
        if i == 0:
            arrived(at_chain("oc", h, z), o_chain.at[base + z], below)
            arrived(at_chain("oc", h, n_z), o_chain.at[base + n_z], above)
            combined(
                h, "o", z, (sides_in, 2 * index), (sides_in, 2 * index + 1), (o_chain, base + z), (o_chain, base + n_z),
                target=h * rows,
            )
        else:
            arrived(at_chain("oc", h, p.zz), o_chain.at[base + p.zz], p.has_out)
            spot = combined(h, "o", p.zz, (sides_in, 2 * index), (sides_in, 2 * index + 1), (o_chain, base + p.zz))
            start(at_chain("oc", h, slot_at(p)), part.at[spot], o_chain.at[base + slot_at(p)], to_z(p.back))

    steps = {
        "own": send_own, "clear": clear, "x": take_x, "y": take_y, "xy": take_xy, "o": take_o, "d": take_d,
        "C": product, "Rd": give_d, "Rx": give_x, "Ry": give_y, "Rxy": give_xy, "Ro": give_o,
    }
    for name, *numbers in PLAN:
        steps[name](*numbers)
    for condition, copy in sent[-SENDS:]:
        when(condition, copy.wait_send)


RECV = {kind: (lambda n_z, batches: n_z * batches) for kind in ("x", "y", "o", "d", "sides")}
RECV["halves"] = RECV["dx"] = RECV["dy"] = lambda n_z, batches: (n_z - n_z // 2) * batches
RECV["core"] = RECV["p"] = lambda n_z, batches: 4 * batches
RECV["dc"] = RECV["oc"] = lambda n_z, batches: (n_z + 1) * batches
SENDS = 40

BATCHES = 2

PLAN = (
    ("own", 0),
    ("clear",),
    ("own", 1),
    ("x", 0, 0),
    ("y", 0, 0),
    ("o", 0, 1),
    ("o", 0, 2),
    ("x", 1, 0),
    ("y", 1, 0),
    ("d", 0, 0),
    ("o", 0, 3),
    ("y", 0, 1),
    ("o", 1, 1),
    ("x", 0, 1),
    ("C", 0, "o"),
    ("y", 0, 2),
    ("d", 0, 1),
    ("d", 0, 2),
    ("x", 0, 2),
    ("y", 0, 3),
    ("x", 0, 3),
    ("o", 1, 3),
    ("d", 0, 3),
    ("C", 0, "y"),
    ("o", 1, 2),
    ("d", 1, 0),
    ("y", 1, 1),
    ("C", 0, "d"),
    ("y", 1, 3),
    ("x", 1, 3),
    ("C", 0, "x"),
    ("Rd", 0, 3),
    ("Ry", 0, 2),
    ("Ry", 0, 1),
    ("d", 1, 2),
    ("d", 1, 1),
    ("Rd", 0, 2),
    ("d", 1, 3),
    ("Rx", 0, 1),
    ("Rd", 0, 1),
    ("x", 1, 2),
    ("y", 1, 2),
    ("Rx", 0, 2),
    ("x", 1, 1),
    ("C", 1, "d"),
    ("Rx", 0, 3),
    ("C", 1, "x"),
    ("Rd", 1, 3),
    ("Rd", 1, 2),
    ("Ry", 0, 3),
    ("C", 1, "y"),
    ("Ro", 0, 2),
    ("Rd", 0, 0),
    ("Rx", 1, 3),
    ("Rx", 1, 2),
    ("Rx", 1, 1),
    ("Rd", 1, 1),
    ("Ry", 1, 3),
    ("Ry", 1, 2),
    ("Ry", 1, 1),
    ("C", 1, "o"),
    ("Ro", 0, 3),
    ("Ro", 1, 3),
    ("Rd", 1, 0),
    ("Rx", 0, 0),
    ("Ry", 0, 0),
    ("Ro", 1, 2),
    ("Ro", 0, 1),
    ("Ro", 1, 1),
    ("Rx", 1, 0),
    ("Ry", 1, 0),
    ("Ro", 0, 0),
    ("Ro", 1, 0),
)


def fused_device(tokens, expert_ids, gate_logits, w_gate, w_up, w_down):
    n_rows, width = tokens.shape
    hidden_width = w_gate.shape[2]
    n_exp = lax.axis_size("expert")
    n_z = n_exp // 2
    batches = BATCHES
    rows = n_rows // batches
    lanes = round_up(width + 2 * n_exp, LANES)
    total = n_exp * lax.axis_size("dp") * batches
    receives = sum(size(n_z, batches) for size in RECV.values())
    bf16 = jnp.bfloat16
    in_vmem = pl.BlockSpec(memory_space=pltpu.VMEM)
    anywhere = pl.BlockSpec(memory_space=pl.ANY)
    return pl.pallas_call(
        functools.partial(fused_kernel, n_exp),
        in_specs=[anywhere] * 6,
        out_specs=in_vmem,
        out_shape=pltpu.VMEM((n_rows, width), bf16),
        scratch_shapes=[
            pltpu.VMEM(expert_ids.shape[::-1], jnp.int32),
            pltpu.VMEM(gate_logits.shape[::-1], jnp.float32),
            pltpu.VMEM((n_rows, width), bf16),
            pltpu.VMEM((total, rows, lanes), bf16),
            pltpu.VMEM((total, rows, width), bf16),
            pltpu.VMEM((total // 2, rows, width), bf16),
            pltpu.VMEM((batches * n_z * 2, rows, width), bf16),
            pltpu.VMEM((batches * n_z, rows // 2, width), bf16),
            pltpu.VMEM((batches * n_z, rows // 2, width), bf16),
            pltpu.VMEM((batches * (n_z + 1), rows, width), bf16),
            pltpu.VMEM((batches * (n_z + 1), rows, width), bf16),
            pltpu.VMEM((width, hidden_width), bf16),
            pltpu.VMEM((width, hidden_width), bf16),
            pltpu.VMEM((width, hidden_width), bf16),
            pltpu.SemaphoreType.DMA((SENDS,)),
            pltpu.SemaphoreType.DMA((receives,)),
            pltpu.SemaphoreType.DMA((6,)),
        ],
        compiler_params=pltpu.CompilerParams(
            collective_id=0, has_side_effects=True, vmem_limit_bytes=60 * 1024 * 1024
        ),
    )(tokens, expert_ids.T, gate_logits.T, w_gate[0], w_up[0], w_down[0].T)


def solution(mesh):
    def per_device(tokens, expert_ids, *others):
        n_exp = lax.axis_size("expert")
        if n_exp > 4 * expert_ids.shape[1]:
            return sparse_device(tokens, expert_ids, *others)
        paired = lax.axis_size("dp") == 4 and n_exp % 2 == 0 and tokens.shape[0] % 32 == 0
        return (fused_device if paired else dense_device)(tokens, expert_ids, *others)

    return jax.shard_map(
        per_device,
        mesh=mesh,
        in_specs=(
            P(("expert", "dp"), None),
            P(("expert", "dp"), None),
            P(("expert", "dp"), None),
            P("expert", None, "dp"),
            P("expert", None, "dp"),
            P("expert", "dp", None),
        ),
        out_specs=P(("expert", "dp"), None),
        check_vma=False,
    )
```
